512 devices in a mesh: space: 128 (over y, z, core), tm: 4 (over x).
Axes of the slice: x: 4, y: 8, z: 8, core: 2. Of those that a mesh axis runs over, the one named last changes fastest.
Arguments:
- snapshots: float32 [262144, 1024], P('space', 'tm'), may hold values from -6 to 6
- final_snapshot: float32 [262144], P('space'), may hold values from -6 to 6
- pod_modes: float32 [262144, 200], P('space'), may hold values from -0.01171875 to 0.01171875
- right_vectors: float32 [1024, 200], P('tm'), may hold values from -0.1875 to 0.1875
- inverse_sing: float32 [200], replicated, may hold values from 0.5 to 2
- eigen_vectors: float32 [200, 200], replicated, may hold values from -0.4375 to 0.4375
Outputs:
- reduced_operator: float32 [200, 200], replicated
- dmd_modes: float32 [262144, 200], P(('space', 'tm'))
The draws below stay inside these ranges and needn't reach their ends.
All inputs are finite; a program needn't handle non-finite values.
Results may differ from the reference program's by a relative error of at most 0.000092.
Values sent between devices are 32-bit elements; how exact they have to be, the bound alone decides.
No kernel may reach another device: no remote copies, remote signals or barrier semaphores. Data moves between devices by JAX's collectives and lax.ppermute only.
A program may use at most 64 MiB of HBM per device.

```python
import math
import jax
import jax.numpy as jnp
from jax import lax

RANK = 200
NPTS = 262144
SNAPS = 1024


def block_scale(stream_key, dims, split, least, top_value):
    def one(position, parts):
        draws = jax.random.uniform(jax.random.fold_in(jax.random.fold_in(stream_key, 6), position), (parts,), jnp.float32, least / len(split), top_value / len(split))
        return jnp.repeat(jnp.exp(draws), dims[position] // parts).reshape((-1,) + (1,) * (len(dims) - position - 1))

    level = one(*split[0])
    for cut in split[1:]:
        level = level * one(*cut)
    return level


def scatter_about(key, dims, width, most, cuts=(), held_as=jnp.bfloat16):
    entries = width * jax.random.normal(key, dims, jnp.float32)
    if cuts:
        entries = entries * block_scale(key, dims, cuts, -0.22, 0.18)
    return jnp.clip(entries, -most, most).astype(held_as)


def setup_inputs(seed: int = 0) -> dict:
    streams_of = jax.random.split(jax.random.key(seed), 7)
    snapshots = scatter_about(streams_of[0], (NPTS, SNAPS), 1.0, 6.0, ((0, 128), (1, 4)), jnp.float32)
    final_snapshot = scatter_about(streams_of[1], (NPTS,), 1.0, 6.0, ((0, 128),), jnp.float32)
    pod_modes = scatter_about(streams_of[2], (NPTS, RANK), NPTS ** -0.5, 0.01171875, ((0, 128),), jnp.float32)
    right_vectors = scatter_about(streams_of[3], (SNAPS, RANK), SNAPS ** -0.5, 0.1875, ((0, 4),), jnp.float32)
    inverse_sing = jnp.clip(jnp.exp(jax.random.uniform(streams_of[4], (RANK,), jnp.float32, math.log(0.5), math.log(2.0))), 0.5, 2.0)
    eigen_vectors = scatter_about(streams_of[5], (RANK, RANK), RANK ** -0.5, 0.4375, (), jnp.float32)
    return {"snapshots": snapshots, "final_snapshot": final_snapshot, "pod_modes": pod_modes, "right_vectors": right_vectors, "inverse_sing": inverse_sing, "eigen_vectors": eigen_vectors}


def reference(snapshots, final_snapshot, pod_modes, right_vectors, inverse_sing, eigen_vectors):
    hi = lax.Precision.HIGHEST
    raised = jnp.concatenate([jnp.zeros((1, RANK), jnp.float32), right_vectors[:-1]], axis=0)
    projected = jnp.dot(snapshots, raised, precision=hi, preferred_element_type=jnp.float32)
    projected = projected + final_snapshot[:, None] * right_vectors[-1][None, :]
    scaled = projected * inverse_sing[None, :]
    reduced_operator = jnp.dot(pod_modes.T, scaled, precision=hi, preferred_element_type=jnp.float32)
    dmd_modes = jnp.dot(scaled, eigen_vectors, precision=hi, preferred_element_type=jnp.float32)
    return reduced_operator, dmd_modes
```

```python
import jax
import jax.numpy as jnp
from jax import lax
from jax.sharding import Mesh
from jax.sharding import PartitionSpec as P

AXES = ("y_far", "y_near", "z", "core", "tm")
SPACE = ("y_far", "y_near", "z", "core")
NEAR = ("y_near", "core", "tm")
FAR = ("y_far", "z")
LANES = 128


def exchanged(tiles, axes):
    return lax.all_to_all(tiles, axes, split_axis=0, concat_axis=0, tiled=True)


def product(a, b, dims):
    return lax.dot_general(
        a, b, (dims, ((), ())), precision=lax.Precision.HIGH, preferred_element_type=jnp.float32
    )


def to_all(value, axes):
    size = lax.axis_size(axes)
    return exchanged(jnp.broadcast_to(value[None], (size, *value.shape)), axes)


def summed_rows(value, blocks):
    share = value.shape[0] // blocks
    half = share // 2
    me = lax.axis_index("tm")

    def rows_of(distance, start, size):
        owner = lax.rem(me + distance, blocks)
        return lax.dynamic_slice_in_dim(value, owner * share + start, size, 0)

    def sent(rows, distance):
        return lax.ppermute(rows, "tm", [(i, (i + distance) % blocks) for i in range(blocks)])

    to_right = jnp.concatenate([rows_of(2, 0, half), rows_of(1, half, half)], axis=0)
    to_left = jnp.concatenate([rows_of(3, 0, half), rows_of(2, half, half)], axis=0)
    from_left, from_right = sent(to_right, 1), sent(to_left, -1)
    top = sent(rows_of(1, 0, half) + from_left[:half], 1)
    bottom = sent(rows_of(3, half, half) + from_right[half:], -1)
    return rows_of(0, 0, share) + jnp.concatenate(
        [from_right[:half] + top, from_left[half:] + bottom], axis=0
    )


def local(snapshots, final_snapshot, pod_modes, right_vectors, inverse_sing, eigen_vectors):
    blocks = lax.axis_size("tm")
    rows, rank = snapshots.shape[0], right_vectors.shape[1]
    before = lax.ppermute(right_vectors[-1], "tm", [(i, (i + 1) % blocks) for i in range(blocks)])
    first = jnp.where(lax.axis_index("tm") == 0, final_snapshot, snapshots[:, 0])
    raised = jnp.concatenate([jnp.zeros((1, rank), jnp.float32), right_vectors[:-1]], axis=0)
    partial_sum = product(snapshots, raised, ((1,), (0,))) + first[:, None] * before[None, :]

    term = product(pod_modes, partial_sum, ((0,), (0,))) * inverse_sing[None, :]
    near = lax.axis_size(NEAR)
    piece = -(-rank * rank // (near * LANES)) * LANES
    flat = jnp.pad(term.reshape(-1), (0, near * piece - rank * rank))
    own = jnp.sum(exchanged(flat.reshape(near, piece), NEAR), axis=0)

    scaled = summed_rows(partial_sum, blocks) * inverse_sing[None, :]
    dmd_modes = product(scaled, eigen_vectors, ((1,), (0,)))

    own = jnp.sum(to_all(own, FAR), axis=0)
    whole = to_all(own, NEAR).reshape(-1)
    return whole[: rank * rank].reshape(rank, rank), dmd_modes


def solution(mesh):
    y = 8
    finer = Mesh(
        mesh.devices.reshape(y // 2, 2, mesh.shape["space"] // (2 * y), 2, mesh.shape["tm"]), AXES
    )
    return jax.shard_map(
        local,
        mesh=finer,
        in_specs=(P(SPACE, "tm"), P(SPACE), P(SPACE, None), P("tm", None), P(), P()),
        out_specs=(P(), P((*SPACE, "tm"), None)),
        check_vma=False,
    )
```

```python
import functools

import jax
import jax.numpy as jnp
from jax import lax
from jax.experimental import pallas as pl
from jax.experimental.pallas import tpu as pltpu
from jax.sharding import Mesh
from jax.sharding import PartitionSpec as P

SPACE = ("y_far", "y_near", "z_far", "z_near", "core")
NEAR = ("y_near", "z_near", "core", "tm")
FAR = ("y_far", "z_far")
LANES = 128
CHUNK = 256
VMEM_GRANT = 16 << 20


def f32(*shape):
    return jax.ShapeDtypeStruct(shape, jnp.float32)


def call(kernel, out, *args, smem=0, hbm=(), scratch=()):
    whole = pl.BlockSpec(memory_space=pltpu.VMEM)
    scalar = pl.BlockSpec(memory_space=pltpu.SMEM)
    outs = out if isinstance(out, tuple) else (out,)
    specs = [scalar] * smem + [whole] * (len(args) - smem)
    args = list(args)
    for i in hbm:
        specs[i] = pl.BlockSpec(memory_space=pltpu.HBM)
        args[i] = pltpu.with_memory_space_constraint(args[i], pltpu.HBM)
    result = pl.pallas_call(
        kernel,
        out_shape=outs,
        in_specs=specs,
        scratch_shapes=scratch,
        out_specs=[whole] * len(outs),
        compiler_params=pltpu.CompilerParams(vmem_limit_bytes=VMEM_GRANT),
    )(*args)
    return result if isinstance(out, tuple) else result[0]


def split(x):
    high = x.astype(jnp.bfloat16)
    return high, (x - high.astype(jnp.float32)).astype(jnp.bfloat16)


def three_pass(a, b):
    dims = (((1,), (1,)), ((), ()))
    dot = functools.partial(
        lax.dot_general, dimension_numbers=dims, preferred_element_type=jnp.float32
    )
    (a_high, a_low), (b_high, b_low) = a, b
    return dot(a_high, b_high) + (dot(a_high, b_low) + dot(a_low, b_high))


def products_kernel(
    at_start, snaps, final, modes, vectors, part, term, snaps_in, final_in, modes_in, vectors_in, sems
):
    rank, snapshots = vectors.shape
    rows = part.shape[0]
    chunks = snaps.shape[0] // CHUNK
    spans = [pl.ds(i * CHUNK, CHUNK) for i in range(chunks)]
    got_vectors = pltpu.make_async_copy(vectors, vectors_in, sems.at[2 * chunks])
    got_final = pltpu.make_async_copy(final, final_in, sems.at[2 * chunks + 1])
    got_snaps = [
        pltpu.make_async_copy(snaps.at[here, :], snaps_in.at[here, :], sems.at[i])
        for i, here in enumerate(spans)
    ]
    got_modes = [
        pltpu.make_async_copy(modes.at[:, here], modes_in.at[:, here], sems.at[chunks + i])
        for i, here in enumerate(spans)
    ]
    got_vectors.start()
    got_snaps[0].start()
    got_final.start()
    got_modes[0].start()
    for i in range(1, chunks):
        got_snaps[i].start()
        got_modes[i].start()

    lane = lax.broadcasted_iota(jnp.int32, (rank, snapshots), 1)
    row = lax.broadcasted_iota(jnp.int32, (rows - rank, snapshots), 0)
    column = lax.broadcasted_iota(jnp.int32, (rows - rank, snapshots), 1)
    unit = jnp.where((row == 0) & (column == 0), 1.0, 0.0)
    got_vectors.wait()
    shifted = jnp.where(lane == 0, 0.0, pltpu.roll(vectors_in[...], 1, 1))
    left = split(jnp.concatenate([shifted, unit], axis=0))
    total = None
    for i, here in enumerate(spans):
        got_snaps[i].wait()
        block = three_pass(left, split(snaps_in[here, :]))
        if i == 0:
            got_final.wait()
        below = lax.broadcasted_iota(jnp.int32, block.shape, 0) == rank
        block = jnp.where(below & (at_start[0] == 1), final_in[:, here], block)
        part[:, here] = block
        got_modes[i].wait()
        product = three_pass(split(modes_in[:, here]), split(block))
        total = product if total is None else total + product
    term[...] = total


def packed_kernel(term, before, sing, out):
    rank = before.shape[1]
    rest = rank - LANES
    column = term[:, rank : rank + 1]
    whole = (term[:, :rank] + column * before[...]) * sing[...]
    out[:rank, :] = whole[:, :LANES]
    tail = jnp.pad(whole[:, LANES:], ((0, 2 * LANES - rank), (0, LANES - rest)))
    for i in range(2):
        turned = tail[i * LANES : (i + 1) * LANES].T
        out[rank + i * rest : rank + (i + 1) * rest, :] = turned[:rest]
    out[rank + 2 * rest :, :] = jnp.zeros((out.shape[0] - rank - 2 * rest, LANES), jnp.float32)


def unpacked_kernel(packed, out):
    rank = out.shape[0]
    rest = rank - LANES
    out[:, :LANES] = packed[:rank, :]
    for i, size in ((0, LANES), (1, rest)):
        tail = packed[rank + i * rest : rank + (i + 1) * rest, :]
        turned = jnp.pad(tail, ((0, LANES - rest), (0, 0))).T
        out[i * LANES : i * LANES + size, LANES:] = turned[:size, :rest]


def sum_and_copy_kernel(tiles, out, *, size, copies):
    total = tiles[:size, :]
    for i in range(1, tiles.shape[0] // size):
        total = total + tiles[i * size : (i + 1) * size, :]
    for i in range(copies):
        out[i * size : (i + 1) * size, :] = total


def shares_kernel(me, part, before, to_right, to_left, right_later, left_later, own):
    rank = own.shape[0]
    half = right_later.shape[1]
    turned = jnp.concatenate(
        [
            jnp.broadcast_to(before[:, i * LANES : (i + 1) * LANES], (LANES, LANES)).T
            for i in range(2)
        ],
        axis=0,
    )[:rank, :1]

    def columns(distance, side):
        owner = lax.rem(me[0] + distance, 4)
        here = pl.ds(pl.multiple_of(owner * (2 * half) + side * half, half), half)
        return part[:rank, here] + turned * part[rank : rank + 1, here]

    to_right[:, :half] = columns(2, 0)
    to_right[:, half:] = columns(1, 1)
    to_left[:, :half] = columns(3, 0)
    to_left[:, half:] = columns(2, 1)
    right_later[...] = columns(1, 0)
    left_later[...] = columns(3, 1)
    own[:, :half] = columns(0, 0)
    own[:, half:] = columns(0, 1)


def exchanged(tiles, axes):
    pieces = lax.axis_size(axes)
    got = lax.all_to_all(tiles.reshape(pieces, -1), axes, split_axis=0, concat_axis=0, tiled=True)
    return got.reshape(tiles.shape)


def step(snapshots, final_snapshot, pod_modes, right_vectors, inverse_sing, eigen_vectors):
    blocks = lax.axis_size("tm")
    rows, rank = snapshots.shape[0], right_vectors.shape[1]
    half = rows // (2 * blocks)
    me = lax.axis_index("tm")

    def sent(value, distance):
        return lax.ppermute(value, "tm", [(i, (i + distance) % blocks) for i in range(blocks)])

    before = sent(right_vectors[-1], 1)
    at_start = (me == 0).astype(jnp.int32)[None]
    part, term = call(
        products_kernel,
        (f32(rank + 8, rows), f32(rank, rank + 8)),
        at_start,
        snapshots,
        final_snapshot[None, :],
        pod_modes.T,
        right_vectors.T,
        smem=1,
        hbm=(1, 2, 3, 4),
        scratch=(
            pltpu.VMEM(snapshots.shape, jnp.float32),
            pltpu.VMEM((1, rows), jnp.float32),
            pltpu.VMEM((rank, rows), jnp.float32),
            pltpu.VMEM((rank, snapshots.shape[1]), jnp.float32),
            pltpu.SemaphoreType.DMA((2 * (rows // CHUNK) + 2,)),
        ),
    )

    near, far = lax.axis_size(NEAR), lax.axis_size(FAR)
    size = -(-(rank + 2 * (rank - LANES)) // near)
    packed = call(packed_kernel, f32(near * size, LANES), term, before[None, :], inverse_sing[None, :])
    copied = functools.partial(sum_and_copy_kernel, size=size)
    tiles = exchanged(packed, NEAR)
    tiles = call(functools.partial(copied, copies=far), f32(far * size, LANES), tiles)
    tiles = exchanged(tiles, FAR)
    tiles = call(functools.partial(copied, copies=near), f32(near * size, LANES), tiles)
    tiles = exchanged(tiles, NEAR)
    reduced_operator = call(unpacked_kernel, f32(rank, rank), tiles)

    to_right, to_left, right_later, left_later, own = call(
        shares_kernel,
        (f32(rank, 2 * half), f32(rank, 2 * half), f32(rank, half), f32(rank, half), f32(rank, 2 * half)),
        me.astype(jnp.int32)[None],
        part,
        jnp.pad(before, (0, 2 * LANES - rank))[None, :],
        smem=1,
    )
    from_left = sent(to_right, 1)
    from_right = sent(to_left, -1)
    top = sent(right_later + from_left[:, :half], 1)
    bottom = sent(left_later + from_right[:, half:], -1)
    scaled = own + jnp.concatenate(
        [from_right[:, :half] + top, from_left[:, half:] + bottom], axis=1
    )
    scaled = scaled * inverse_sing[:, None]
    dmd_modes = lax.dot_general(
        eigen_vectors,
        scaled,
        (((0,), (0,)), ((), ())),
        precision=lax.Precision.HIGH,
        preferred_element_type=jnp.float32,
    )
    return reduced_operator, dmd_modes.T


def solution(mesh):
    finer = Mesh(mesh.devices.reshape(4, 2, 4, 2, 2, mesh.shape["tm"]), (*SPACE, "tm"))
    return jax.shard_map(
        step,
        mesh=finer,
        in_specs=(P(SPACE, "tm"), P(SPACE), P(SPACE, None), P("tm", None), P(), P()),
        out_specs=(P(), P((*SPACE, "tm"), None)),
        check_vma=False,
    )
```

```python
import functools

import jax
import jax.numpy as jnp
from jax import lax
from jax.experimental import pallas as pl
from jax.experimental.pallas import tpu as pltpu
from jax.sharding import Mesh
from jax.sharding import PartitionSpec as P

SPACE = ("y_far", "y_near", "z_far", "z_near", "core")
NEAR = ("y_near", "z_near", "core", "tm")
FAR = ("y_far", "z_far")
LANES = 128
BLOCKS = 4
EXTRA = 2 * BLOCKS
CHUNK = 512
VMEM_GRANT = 16 << 20


def f32(*shape):
    return jax.ShapeDtypeStruct(shape, jnp.float32)


def call(kernel, out, *args, smem=0, hbm=(), scratch=()):
    whole = pl.BlockSpec(memory_space=pltpu.VMEM)
    scalar = pl.BlockSpec(memory_space=pltpu.SMEM)
    outs = out if isinstance(out, tuple) else (out,)
    specs = [scalar] * smem + [whole] * (len(args) - smem)
    args = list(args)
    for i in hbm:
        specs[i] = pl.BlockSpec(memory_space=pltpu.HBM)
        args[i] = pltpu.with_memory_space_constraint(args[i], pltpu.HBM)
    result = pl.pallas_call(
        kernel,
        out_shape=outs,
        in_specs=specs,
        scratch_shapes=scratch,
        out_specs=[whole] * len(outs),
        compiler_params=pltpu.CompilerParams(vmem_limit_bytes=VMEM_GRANT),
    )(*args)
    return result if isinstance(out, tuple) else result[0]


def split(x):
    high = x.astype(jnp.bfloat16)
    return high, (x - high.astype(jnp.float32)).astype(jnp.bfloat16)


def three_pass(a, b, contract=(1, 1)):
    dims = (((contract[0],), (contract[1],)), ((), ()))
    dot = functools.partial(
        lax.dot_general, dimension_numbers=dims, preferred_element_type=jnp.float32
    )
    (a_high, a_low), (b_high, b_low) = a, b
    return dot(a_high, b_high) + (dot(a_high, b_low) + dot(a_low, b_high))


def shifted(vectors):
    lane = lax.broadcasted_iota(jnp.int32, vectors.shape, 1)
    return jnp.where(lane == 0, 0.0, pltpu.roll(vectors, 1, 1))


def turned(row):
    row = jnp.pad(row, ((0, 0), (0, 2 * LANES - row.shape[1])))
    halves = [
        jnp.broadcast_to(row[:, i * LANES : (i + 1) * LANES], (LANES, LANES)).T[:, :1]
        for i in range(2)
    ]
    return jnp.concatenate(halves, axis=0)


def term_kernel(
    me, snaps, final, modes, vectors, packed, snaps_in, final_in, vectors_in, modes_in, sems
):
    rank, _ = vectors.shape
    chunks = snaps.shape[0] // CHUNK
    spans = [pl.ds(i * CHUNK, CHUNK) for i in range(chunks)]
    got_modes = [
        pltpu.make_async_copy(modes.at[:, here], modes_in.at[:, here], sems.at[i])
        for i, here in enumerate(spans)
    ]
    got_snaps = [
        pltpu.make_async_copy(snaps.at[here, :], snaps_in.at[here, :], sems.at[chunks + i])
        for i, here in enumerate(spans)
    ]
    got_final = pltpu.make_async_copy(final, final_in, sems.at[2 * chunks])
    got_vectors = pltpu.make_async_copy(vectors, vectors_in, sems.at[2 * chunks + 1])
    for i in range(chunks):
        got_modes[i].start()
        got_snaps[i].start()
    got_final.start()
    got_vectors.start()

    total = of_final = None
    for i, here in enumerate(spans):
        got_modes[i].wait()
        got_snaps[i].wait()
        left = split(modes_in[:, here])
        product = three_pass(left, split(snaps_in[here, :]), (1, 0))
        if i == 0:
            got_final.wait()
        column = three_pass(left, split(jnp.broadcast_to(final_in[:, here], (8, CHUNK))))
        total = product if total is None else total + product
        of_final = column if of_final is None else of_final + column
    got_vectors.wait()
    whole = three_pass(split(total), split(shifted(vectors_in[...])))
    first = jnp.where(me[0] == 0, of_final[:, :1], total[:, :1])
    packed[:rank, :] = whole[:, :LANES]
    rest = rank - LANES
    tail = jnp.pad(whole[:, LANES:], ((0, 0), (0, LANES - rest)))
    lane = lax.broadcasted_iota(jnp.int32, tail.shape, 1)
    tail = jnp.where(lane == rest + me[0], first, tail)
    tail = jnp.pad(tail, ((0, 2 * LANES - rank), (0, 0)))
    used = rest + BLOCKS
    for i in range(2):
        turn = tail[i * LANES : (i + 1) * LANES].T
        packed[rank + i * used : rank + (i + 1) * used, :] = turn[:used]


def shares_kernel(
    me, snaps, final, vectors, to_right, to_left, right_later, left_later, own
):
    rank, snapshots = vectors.shape
    half = right_later.shape[1]
    row = lax.broadcasted_iota(jnp.int32, (EXTRA, snapshots), 0)
    column = lax.broadcasted_iota(jnp.int32, (EXTRA, snapshots), 1)
    unit = jnp.where((row == me[0]) & (column == 0), 1.0, 0.0)
    left = split(jnp.concatenate([shifted(vectors[...]), unit], axis=0))
    tail = jnp.pad(vectors[:, snapshots - LANES :], ((0, 2 * LANES - rank), (0, 0)))
    last = jnp.concatenate([tail[:LANES].T[LANES - 1 :], tail[LANES:].T[LANES - 1 :]], axis=1)
    slot = lax.broadcasted_iota(jnp.int32, (EXTRA, half), 0)
    after = BLOCKS + lax.rem(me[0] + 1, BLOCKS)

    def write(out, at, distance, side):
        owner = lax.rem(me[0] + distance, BLOCKS)
        here = pl.ds(pl.multiple_of(owner * (2 * half) + side * half, half), half)
        block = three_pass(left, split(snaps[here, :]))
        extra = jnp.where((slot == me[0]) & (me[0] == 0), final[:, here], block[rank:])
        there = slice(at * half, (at + 1) * half)
        out[:rank, there] = block[:rank]
        out[rank:, there] = jnp.where(slot == after, last, extra)

    write(to_right, 0, 2, 0)
    write(to_right, 1, 1, 1)
    write(to_left, 0, 3, 0)
    write(to_left, 1, 2, 1)
    write(right_later, 0, 1, 0)
    write(left_later, 0, 3, 1)
    write(own, 0, 0, 0)
    write(own, 1, 0, 1)


def add_kernel(later, arrived, out, *, side):
    half = out.shape[1]
    out[...] = later[...] + arrived[:, side * half : (side + 1) * half]


def sum_and_copy_kernel(tiles, out, *, size, copies):
    total = tiles[:size, :]
    for i in range(1, tiles.shape[0] // size):
        total = total + tiles[i * size : (i + 1) * size, :]
    for i in range(copies):
        out[i * size : (i + 1) * size, :] = total


def dmd_kernel(own, from_right, from_left, top, bottom, sing, vectors, out, rows):
    rank = out.shape[0]
    half = top.shape[1]
    scale = turned(sing[...])[:rank]
    right = split(vectors[...])
    for i, arrived in ((0, from_right[:, :half] + top[...]), (1, from_left[:, half:] + bottom[...])):
        there = slice(i * half, (i + 1) * half)
        total = own[:, there] + arrived
        first = total[rank : rank + BLOCKS]
        last = total[rank + BLOCKS :, :rank]
        if i == 0:
            rows[...] = last
        summed = total[:rank] + three_pass(split(last), split(first), (0, 0))
        out[:, there] = three_pass(right, split(summed * scale), (0, 0))


def operator_kernel(packed, rows, sing, out):
    rank = out.shape[0]
    rest = rank - LANES
    used = rest + BLOCKS
    first = jnp.concatenate(
        [
            packed[rank + rest : rank + used, :],
            packed[rank + used + rest : rank + 2 * used, :][:, :rest],
        ],
        axis=1,
    )
    term = three_pass(split(first), split(rows[...]), (0, 0))
    scale = sing[...]
    out[:, :LANES] = (packed[:rank, :] + term[:, :LANES]) * scale[:, :LANES]
    for i, size in ((0, LANES), (1, rest)):
        tail = packed[rank + i * used : rank + i * used + rest, :]
        turn = jnp.pad(tail, ((0, LANES - rest), (0, 0))).T[:size, :rest]
        here = slice(i * LANES, i * LANES + size)
        out[here, LANES:] = (turn + term[here, LANES:]) * scale[:, LANES:]


def exchanged(tiles, axes):
    pieces = lax.axis_size(axes)
    got = lax.all_to_all(tiles.reshape(pieces, -1), axes, split_axis=0, concat_axis=0, tiled=True)
    return got.reshape(tiles.shape)


def step(snapshots, final_snapshot, pod_modes, right_vectors, inverse_sing, eigen_vectors):
    blocks = lax.axis_size("tm")
    rows, rank = snapshots.shape[0], right_vectors.shape[1]
    half = rows // (2 * blocks)
    me = lax.axis_index("tm").astype(jnp.int32)[None]
    sing = inverse_sing[None, :]

    def sent(value, distance):
        return lax.ppermute(value, "tm", [(i, (i + distance) % blocks) for i in range(blocks)])

    near, far = lax.axis_size(NEAR), lax.axis_size(FAR)
    lines = rank + 2 * (rank - LANES + BLOCKS)
    size = lines // near
    packed, snaps_in, final_in, vectors_in = call(
        term_kernel,
        (
            f32(lines, LANES),
            pltpu.VMEM(snapshots.shape, jnp.float32),
            pltpu.VMEM((1, rows), jnp.float32),
            pltpu.VMEM((rank, snapshots.shape[1]), jnp.float32),
        ),
        me,
        snapshots,
        final_snapshot[None, :],
        pod_modes.T,
        right_vectors.T,
        smem=1,
        hbm=(1, 2, 3, 4),
        scratch=(
            pltpu.VMEM((rank, rows), jnp.float32),
            pltpu.SemaphoreType.DMA((2 * (rows // CHUNK) + 2,)),
        ),
    )
    tiles = exchanged(packed, NEAR)

    to_right, to_left, right_later, left_later, own = call(
        shares_kernel,
        tuple(f32(rank + EXTRA, n * half) for n in (2, 2, 1, 1, 2)),
        me,
        snaps_in,
        final_in,
        vectors_in,
        smem=1,
    )
    from_left = sent(to_right, 1)
    from_right = sent(to_left, -1)

    copied = functools.partial(sum_and_copy_kernel, size=size)
    tiles = call(functools.partial(copied, copies=far), f32(far * size, LANES), tiles)
    tiles = exchanged(tiles, FAR)
    added = f32(rank + EXTRA, half)
    top = sent(call(functools.partial(add_kernel, side=0), added, right_later, from_left), 1)
    bottom = sent(call(functools.partial(add_kernel, side=1), added, left_later, from_right), -1)

    tiles = call(functools.partial(copied, copies=near), f32(near * size, LANES), tiles)
    tiles = exchanged(tiles, NEAR)
    dmd_modes, last_rows = call(
        dmd_kernel,
        (f32(rank, 2 * half), f32(BLOCKS, rank)),
        own,
        from_right,
        from_left,
        top,
        bottom,
        sing,
        eigen_vectors,
    )
    reduced_operator = call(operator_kernel, f32(rank, rank), tiles, last_rows, sing)
    return reduced_operator, dmd_modes.T


def solution(mesh):
    finer = Mesh(mesh.devices.reshape(4, 2, 4, 2, 2, mesh.shape["tm"]), (*SPACE, "tm"))
    return jax.shard_map(
        step,
        mesh=finer,
        in_specs=(P(SPACE, "tm"), P(SPACE), P(SPACE, None), P("tm", None), P(), P()),
        out_specs=(P(), P((*SPACE, "tm"), None)),
        check_vma=False,
    )
```

```python
import functools

import jax
import jax.numpy as jnp
from jax import lax
from jax.experimental import pallas as pl
from jax.experimental.pallas import tpu as pltpu
from jax.sharding import Mesh
from jax.sharding import PartitionSpec as P

SPACE = ("y_far", "y_near", "z_far", "z_near", "core")
NEAR = ("y_near", "z_near", "core", "tm")
FAR = ("y_far", "z_far")
LANES = 128
BLOCKS = 4
EXTRA = 2 * BLOCKS
CHUNK = 512
VMEM_GRANT = 16 << 20


def f32(*shape):
    return jax.ShapeDtypeStruct(shape, jnp.float32)


def call(kernel, out, *args, smem=0, hbm=(), scratch=()):
    whole = pl.BlockSpec(memory_space=pltpu.VMEM)
    scalar = pl.BlockSpec(memory_space=pltpu.SMEM)
    outs = out if isinstance(out, tuple) else (out,)
    specs = [scalar] * smem + [whole] * (len(args) - smem)
    args = list(args)
    for i in hbm:
        specs[i] = pl.BlockSpec(memory_space=pltpu.HBM)
        args[i] = pltpu.with_memory_space_constraint(args[i], pltpu.HBM)
    result = pl.pallas_call(
        kernel,
        out_shape=outs,
        in_specs=specs,
        scratch_shapes=scratch,
        out_specs=[whole] * len(outs),
        compiler_params=pltpu.CompilerParams(vmem_limit_bytes=VMEM_GRANT),
    )(*args)
    return result if isinstance(out, tuple) else result[0]


def split(x):
    high = x.astype(jnp.bfloat16)
    return high, (x - high.astype(jnp.float32)).astype(jnp.bfloat16)


def three_pass(a, b, contract=(1, 1)):
    dims = (((contract[0],), (contract[1],)), ((), ()))
    dot = functools.partial(
        lax.dot_general, dimension_numbers=dims, preferred_element_type=jnp.float32
    )
    (a_high, a_low), (b_high, b_low) = a, b
    return dot(a_high, b_high) + (dot(a_high, b_low) + dot(a_low, b_high))


def shifted(vectors):
    lane = lax.broadcasted_iota(jnp.int32, vectors.shape, 1)
    return jnp.where(lane == 0, 0.0, pltpu.roll(vectors, 1, 1))


def turned(row):
    row = jnp.pad(row, ((0, 0), (0, 2 * LANES - row.shape[1])))
    halves = [
        jnp.broadcast_to(row[:, i * LANES : (i + 1) * LANES], (LANES, LANES)).T[:, :1]
        for i in range(2)
    ]
    return jnp.concatenate(halves, axis=0)


def term_kernel(
    me, snaps, final, modes, vectors, packed, snaps_in, final_in, vectors_in, modes_in, sems
):
    rank, _ = vectors.shape
    chunks = snaps.shape[0] // CHUNK
    spans = [pl.ds(i * CHUNK, CHUNK) for i in range(chunks)]
    got_modes = [
        pltpu.make_async_copy(modes.at[:, here], modes_in.at[:, here], sems.at[i])
        for i, here in enumerate(spans)
    ]
    got_snaps = [
        pltpu.make_async_copy(snaps.at[here, :], snaps_in.at[here, :], sems.at[chunks + i])
        for i, here in enumerate(spans)
    ]
    got_final = pltpu.make_async_copy(final, final_in, sems.at[2 * chunks])
    got_vectors = pltpu.make_async_copy(vectors, vectors_in, sems.at[2 * chunks + 1])
    for i in range(chunks):
        got_modes[i].start()
        got_snaps[i].start()
    got_final.start()
    got_vectors.start()

    total = of_final = None
    for i, here in enumerate(spans):
        got_modes[i].wait()
        got_snaps[i].wait()
        left = split(modes_in[:, here])
        product = three_pass(left, split(snaps_in[here, :]), (1, 0))
        if i == 0:
            got_final.wait()
        column = three_pass(left, split(jnp.broadcast_to(final_in[:, here], (8, CHUNK))))
        total = product if total is None else total + product
        of_final = column if of_final is None else of_final + column
    got_vectors.wait()
    whole = three_pass(split(total), split(shifted(vectors_in[...])))
    first = jnp.where(me[0] == 0, of_final[:, :1], total[:, :1])
    packed[:rank, :] = whole[:, :LANES]
    rest = rank - LANES
    tail = jnp.pad(whole[:, LANES:], ((0, 0), (0, LANES - rest)))
    lane = lax.broadcasted_iota(jnp.int32, tail.shape, 1)
    tail = jnp.where(lane == rest + me[0], first, tail)
    tail = jnp.pad(tail, ((0, 2 * LANES - rank), (0, 0)))
    used = rest + BLOCKS
    for i in range(2):
        turn = tail[i * LANES : (i + 1) * LANES].T
        packed[rank + i * used : rank + (i + 1) * used, :] = turn[:used]


def shares_of(me, snaps, final, vectors):
    rank, snapshots = vectors.shape
    points = snaps.shape[0]
    row = lax.broadcasted_iota(jnp.int32, (EXTRA, snapshots), 0)
    column = lax.broadcasted_iota(jnp.int32, (EXTRA, snapshots), 1)
    unit = jnp.where((row == me) & (column == 0), 1.0, 0.0)
    left = split(jnp.concatenate([shifted(vectors), unit], axis=0))
    tail = jnp.pad(vectors[:, snapshots - LANES :], ((0, 2 * LANES - rank), (0, 0)))
    last = [tail[:LANES].T[LANES - 1 :], tail[LANES:].T[LANES - 1 :]]
    last = jnp.concatenate(last * (points // (2 * LANES)), axis=1)
    block = three_pass(left, split(snaps))
    slot = lax.broadcasted_iota(jnp.int32, (EXTRA, points), 0)
    extra = jnp.where((slot == me) & (me == 0), final, block[rank:])
    extra = jnp.where(slot == BLOCKS + lax.rem(me + 1, BLOCKS), last, extra)
    return block[:rank], extra


def share_kernel(me, snaps, final, vectors, out, *, distance):
    rank, points = vectors.shape[0], out.shape[1]
    owner = lax.rem(me[0] + distance, BLOCKS)
    here = pl.ds(pl.multiple_of(owner * points, points), points)
    out[:rank, :], out[rank:, :] = shares_of(me[0], snaps[here, :], final[:, here], vectors[...])


def add_kernel(own, arrived, out):
    out[...] = own[...] + arrived[...]


def sum_and_copy_kernel(tiles, out, *, size, copies):
    total = tiles[:size, :]
    for i in range(1, tiles.shape[0] // size):
        total = total + tiles[i * size : (i + 1) * size, :]
    for i in range(copies):
        out[i * size : (i + 1) * size, :] = total


def dmd_kernel(
    me, snaps, final, vectors, from_right, from_left, sing, eigen, out, rows, snaps_in, final_in, vectors_in, sems
):
    rank, points = out.shape
    here = pl.ds(pl.multiple_of(me[0] * points, points), points)
    copies = (
        pltpu.make_async_copy(vectors, vectors_in, sems.at[0]),
        pltpu.make_async_copy(snaps.at[here, :], snaps_in, sems.at[1]),
        pltpu.make_async_copy(final.at[:, here], final_in, sems.at[2]),
    )
    for copy in copies:
        copy.start()
    scale = turned(sing[...])[:rank]
    right = split(eigen[...])
    arrived = from_right[...] + from_left[...]
    for copy in copies:
        copy.wait()
    block, extra = shares_of(me[0], snaps_in[...], final_in[...], vectors_in[...])
    extra = extra + arrived[rank:]
    last = extra[BLOCKS:, :rank]
    rows[...] = last
    summed = block + arrived[:rank] + three_pass(split(last), split(extra[:BLOCKS]), (0, 0))
    out[...] = three_pass(right, split(summed * scale), (0, 0))


def operator_kernel(packed, rows, sing, out):
    rank = out.shape[0]
    rest = rank - LANES
    used = rest + BLOCKS
    first = jnp.concatenate(
        [
            packed[rank + rest : rank + used, :],
            packed[rank + used + rest : rank + 2 * used, :][:, :rest],
        ],
        axis=1,
    )
    term = three_pass(split(first), split(rows[...]), (0, 0))
    scale = sing[...]
    out[:, :LANES] = (packed[:rank, :] + term[:, :LANES]) * scale[:, :LANES]
    for i, size in ((0, LANES), (1, rest)):
        tail = packed[rank + i * used : rank + i * used + rest, :]
        turn = jnp.pad(tail, ((0, LANES - rest), (0, 0))).T[:size, :rest]
        here = slice(i * LANES, i * LANES + size)
        out[here, LANES:] = (turn + term[here, LANES:]) * scale[:, LANES:]


def exchanged(tiles, axes):
    pieces = lax.axis_size(axes)
    got = lax.all_to_all(tiles.reshape(pieces, -1), axes, split_axis=0, concat_axis=0, tiled=True)
    return got.reshape(tiles.shape)


def step(snapshots, final_snapshot, pod_modes, right_vectors, inverse_sing, eigen_vectors):
    blocks = lax.axis_size("tm")
    rows, rank = snapshots.shape[0], right_vectors.shape[1]
    half = rows // (2 * blocks)
    me = lax.axis_index("tm").astype(jnp.int32)[None]
    sing = inverse_sing[None, :]

    def sent(value, distance):
        return lax.ppermute(value, "tm", [(i, (i + distance) % blocks) for i in range(blocks)])

    near, far = lax.axis_size(NEAR), lax.axis_size(FAR)
    lines = rank + 2 * (rank - LANES + BLOCKS)
    size = lines // near
    packed, snaps_in, final_in, vectors_in = call(
        term_kernel,
        (
            f32(lines, LANES),
            pltpu.VMEM(snapshots.shape, jnp.float32),
            pltpu.VMEM((1, rows), jnp.float32),
            pltpu.VMEM((rank, snapshots.shape[1]), jnp.float32),
        ),
        me,
        snapshots,
        final_snapshot[None, :],
        pod_modes.T,
        right_vectors.T,
        smem=1,
        hbm=(1, 2, 3, 4),
        scratch=(
            pltpu.VMEM((rank, rows), jnp.float32),
            pltpu.SemaphoreType.DMA((2 * (rows // CHUNK) + 2,)),
        ),
    )
    tiles = exchanged(packed, NEAR)

    share = f32(rank + EXTRA, 2 * half)

    def share_for(distance):
        kernel = functools.partial(share_kernel, distance=distance)
        return call(kernel, share, me, snaps_in, final_in, vectors_in, smem=1)

    two_right, left, one_right = share_for(2), share_for(3), share_for(1)
    from_left = sent(two_right, 1)

    copied = functools.partial(sum_and_copy_kernel, size=size)
    tiles = call(functools.partial(copied, copies=far), f32(far * size, LANES), tiles)
    tiles = exchanged(tiles, FAR)
    from_left = sent(call(add_kernel, share, one_right, from_left), 1)
    from_right = sent(left, -1)

    tiles = call(functools.partial(copied, copies=near), f32(near * size, LANES), tiles)
    tiles = exchanged(tiles, NEAR)
    dmd_modes, last_rows = call(
        dmd_kernel,
        (f32(rank, 2 * half), f32(BLOCKS, rank)),
        me,
        snapshots,
        final_snapshot[None, :],
        right_vectors.T,
        from_right,
        from_left,
        sing,
        eigen_vectors,
        smem=1,
        hbm=(1, 2, 3),
        scratch=(
            pltpu.VMEM((2 * half, snapshots.shape[1]), jnp.float32),
            pltpu.VMEM((1, 2 * half), jnp.float32),
            pltpu.VMEM((rank, snapshots.shape[1]), jnp.float32),
            pltpu.SemaphoreType.DMA((3,)),
        ),
    )
    reduced_operator = call(operator_kernel, f32(rank, rank), tiles, last_rows, sing)
    return reduced_operator, dmd_modes.T


def solution(mesh):
    finer = Mesh(mesh.devices.reshape(4, 2, 4, 2, 2, mesh.shape["tm"]), (*SPACE, "tm"))
    return jax.shard_map(
        step,
        mesh=finer,
        in_specs=(P(SPACE, "tm"), P(SPACE), P(SPACE, None), P("tm", None), P(), P()),
        out_specs=(P(), P((*SPACE, "tm"), None)),
        check_vma=False,
    )
```

```python
import functools

import jax
import jax.numpy as jnp
import numpy as np
from jax import lax
from jax.experimental import pallas as pl
from jax.experimental.pallas import tpu as pltpu
from jax.sharding import Mesh
from jax.sharding import PartitionSpec as P

SPACE = ("y_far", "y_near", "z_far", "z_near", "core")
ALL = (*SPACE, "tm")
NEAR = ("y_near", "z_near", "core", "tm")
FAR = ("y_far", "z_far")
NEAR_FIRST = (1, 1, 1, 2)
FAR_FIRST = (2, 3)
LANES = 128
BLOCKS = 4
EXTRA = 2 * BLOCKS
CHUNK = 512
VMEM_GRANT = 16 << 20


def f32(*shape):
    return jax.ShapeDtypeStruct(shape, jnp.float32)


def call(kernel, out, *args, smem=0, hbm=(), scratch=()):
    whole = pl.BlockSpec(memory_space=pltpu.VMEM)
    scalar = pl.BlockSpec(memory_space=pltpu.SMEM)
    outs = out if isinstance(out, tuple) else (out,)
    specs = [scalar] * smem + [whole] * (len(args) - smem)
    args = list(args)
    for i in hbm:
        specs[i] = pl.BlockSpec(memory_space=pltpu.HBM)
        args[i] = pltpu.with_memory_space_constraint(args[i], pltpu.HBM)
    result = pl.pallas_call(
        kernel,
        out_shape=outs,
        in_specs=specs,
        scratch_shapes=scratch,
        out_specs=[whole] * len(outs),
        compiler_params=pltpu.CompilerParams(vmem_limit_bytes=VMEM_GRANT),
    )(*args)
    return result if isinstance(out, tuple) else result[0]


def split(x):
    high = x.astype(jnp.bfloat16)
    return high, (x - high.astype(jnp.float32)).astype(jnp.bfloat16)


def three_pass(a, b, contract=(1, 1)):
    dims = (((contract[0],), (contract[1],)), ((), ()))
    dot = functools.partial(
        lax.dot_general, dimension_numbers=dims, preferred_element_type=jnp.float32
    )
    (a_high, a_low), (b_high, b_low) = a, b
    return dot(a_high, b_high) + (dot(a_high, b_low) + dot(a_low, b_high))


def shifted(vectors):
    lane = lax.broadcasted_iota(jnp.int32, vectors.shape, 1)
    return jnp.where(lane == 0, 0.0, pltpu.roll(vectors, 1, 1))


def turned(row):
    row = jnp.pad(row, ((0, 0), (0, 2 * LANES - row.shape[1])))
    halves = [
        jnp.broadcast_to(row[:, i * LANES : (i + 1) * LANES], (LANES, LANES)).T[:, :1]
        for i in range(2)
    ]
    return jnp.concatenate(halves, axis=0)


def term_kernel(
    me, snaps, final, modes, vectors, packed, snaps_in, final_in, vectors_in, modes_in, sems
):
    rank, _ = vectors.shape
    chunks = snaps.shape[0] // CHUNK
    spans = [pl.ds(i * CHUNK, CHUNK) for i in range(chunks)]
    got_modes = [
        pltpu.make_async_copy(modes.at[:, here], modes_in.at[:, here], sems.at[i])
        for i, here in enumerate(spans)
    ]
    got_snaps = [
        pltpu.make_async_copy(snaps.at[here, :], snaps_in.at[here, :], sems.at[chunks + i])
        for i, here in enumerate(spans)
    ]
    got_final = pltpu.make_async_copy(final, final_in, sems.at[2 * chunks])
    got_vectors = pltpu.make_async_copy(vectors, vectors_in, sems.at[2 * chunks + 1])
    for i in range(chunks):
        got_modes[i].start()
        got_snaps[i].start()
    got_final.start()
    got_vectors.start()

    total = of_final = None
    for i, here in enumerate(spans):
        got_modes[i].wait()
        got_snaps[i].wait()
        left = split(modes_in[:, here])
        product = three_pass(left, split(snaps_in[here, :]), (1, 0))
        if i == 0:
            got_final.wait()
        column = three_pass(left, split(jnp.broadcast_to(final_in[:, here], (8, CHUNK))))
        total = product if total is None else total + product
        of_final = column if of_final is None else of_final + column
    got_vectors.wait()
    whole = three_pass(split(total), split(shifted(vectors_in[...])))
    first = jnp.where(me[0] == 0, of_final[:, :1], total[:, :1])
    packed[:rank, :] = whole[:, :LANES]
    rest = rank - LANES
    tail = jnp.pad(whole[:, LANES:], ((0, 0), (0, LANES - rest)))
    lane = lax.broadcasted_iota(jnp.int32, tail.shape, 1)
    tail = jnp.where(lane == rest + me[0], first, tail)
    tail = jnp.pad(tail, ((0, 2 * LANES - rank), (0, 0)))
    used = rest + BLOCKS
    for i in range(2):
        turn = tail[i * LANES : (i + 1) * LANES].T
        packed[rank + i * used : rank + (i + 1) * used, :] = turn[:used]


def shares_of(me, snaps, final, vectors):
    rank, snapshots = vectors.shape
    points = snaps.shape[0]
    row = lax.broadcasted_iota(jnp.int32, (EXTRA, snapshots), 0)
    column = lax.broadcasted_iota(jnp.int32, (EXTRA, snapshots), 1)
    unit = jnp.where((row == me) & (column == 0), 1.0, 0.0)
    left = split(jnp.concatenate([shifted(vectors), unit], axis=0))
    tail = jnp.pad(vectors[:, snapshots - LANES :], ((0, 2 * LANES - rank), (0, 0)))
    last = [tail[:LANES].T[LANES - 1 :], tail[LANES:].T[LANES - 1 :]]
    last = jnp.concatenate(last * (points // (2 * LANES)), axis=1)
    block = three_pass(left, split(snaps))
    slot = lax.broadcasted_iota(jnp.int32, (EXTRA, points), 0)
    extra = jnp.where((slot == me) & (me == 0), final, block[rank:])
    extra = jnp.where(slot == BLOCKS + lax.rem(me + 1, BLOCKS), last, extra)
    return block[:rank], extra


def share_kernel(me, snaps, final, vectors, out, *, distance):
    rank, points = vectors.shape[0], out.shape[1]
    owner = lax.rem(me[0] + distance, BLOCKS)
    here = pl.ds(pl.multiple_of(owner * points, points), points)
    out[:rank, :], out[rank:, :] = shares_of(me[0], snaps[here, :], final[:, here], vectors[...])


def add_kernel(own, arrived, out):
    out[...] = own[...] + arrived[...]


def sum_and_copy_kernel(tiles, out, *, size, copies):
    total = tiles[:size, :]
    for i in range(1, tiles.shape[0] // size):
        total = total + tiles[i * size : (i + 1) * size, :]
    for i in range(copies):
        out[i * size : (i + 1) * size, :] = total


def dmd_kernel(
    me, snaps, final, vectors, from_right, from_left, sing, eigen, out, rows, snaps_in, final_in, vectors_in, sems
):
    rank, points = out.shape
    here = pl.ds(pl.multiple_of(me[0] * points, points), points)
    copies = (
        pltpu.make_async_copy(vectors, vectors_in, sems.at[0]),
        pltpu.make_async_copy(snaps.at[here, :], snaps_in, sems.at[1]),
        pltpu.make_async_copy(final.at[:, here], final_in, sems.at[2]),
    )
    for copy in copies:
        copy.start()
    scale = turned(sing[...])[:rank]
    right = split(eigen[...])
    arrived = from_right[...] + from_left[...]
    for copy in copies:
        copy.wait()
    block, extra = shares_of(me[0], snaps_in[...], final_in[...], vectors_in[...])
    extra = extra + arrived[rank:]
    last = extra[BLOCKS:, :rank]
    rows[...] = last
    summed = block + arrived[:rank] + three_pass(split(last), split(extra[:BLOCKS]), (0, 0))
    out[...] = three_pass(right, split(summed * scale), (0, 0))


def operator_kernel(packed, rows, sing, out):
    rank = out.shape[0]
    rest = rank - LANES
    used = rest + BLOCKS
    first = jnp.concatenate(
        [
            packed[rank + rest : rank + used, :],
            packed[rank + used + rest : rank + 2 * used, :][:, :rest],
        ],
        axis=1,
    )
    term = three_pass(split(first), split(rows[...]), (0, 0))
    scale = sing[...]
    out[:, :LANES] = (packed[:rank, :] + term[:, :LANES]) * scale[:, :LANES]
    for i, size in ((0, LANES), (1, rest)):
        tail = packed[rank + i * used : rank + i * used + rest, :]
        turn = jnp.pad(tail, ((0, LANES - rest), (0, 0))).T[:size, :rest]
        here = slice(i * LANES, i * LANES + size)
        out[here, LANES:] = (turn + term[here, LANES:]) * scale[:, LANES:]


def groups_of(axes, first):
    sizes = {axis: lax.axis_size(axis) for axis in ALL}
    places = np.arange(np.prod(list(sizes.values()))).reshape(*sizes.values())
    for axis, start in zip(axes, first, strict=True):
        places = np.roll(places, -start, ALL.index(axis))
    others = [i for i, axis in enumerate(ALL) if axis not in axes]
    places = places.transpose(*others, *(ALL.index(axis) for axis in axes))
    return places.reshape(-1, int(np.prod([sizes[axis] for axis in axes]))).tolist()


def exchanged(tiles, groups):
    pieces = tiles.reshape(len(groups[0]), -1)
    got = lax.all_to_all(
        pieces, ALL, split_axis=0, concat_axis=0, tiled=True, axis_index_groups=groups
    )
    return got.reshape(tiles.shape)


def step(snapshots, final_snapshot, pod_modes, right_vectors, inverse_sing, eigen_vectors):
    blocks = lax.axis_size("tm")
    rows, rank = snapshots.shape[0], right_vectors.shape[1]
    half = rows // (2 * blocks)
    me = lax.axis_index("tm").astype(jnp.int32)[None]
    sing = inverse_sing[None, :]

    def sent(value, distance):
        return lax.ppermute(value, "tm", [(i, (i + distance) % blocks) for i in range(blocks)])

    near, far = lax.axis_size(NEAR), lax.axis_size(FAR)
    near_groups, far_groups = groups_of(NEAR, NEAR_FIRST), groups_of(FAR, FAR_FIRST)
    lines = rank + 2 * (rank - LANES + BLOCKS)
    size = lines // near
    packed, snaps_in, final_in, vectors_in = call(
        term_kernel,
        (
            f32(lines, LANES),
            pltpu.VMEM(snapshots.shape, jnp.float32),
            pltpu.VMEM((1, rows), jnp.float32),
            pltpu.VMEM((rank, snapshots.shape[1]), jnp.float32),
        ),
        me,
        snapshots,
        final_snapshot[None, :],
        pod_modes.T,
        right_vectors.T,
        smem=1,
        hbm=(1, 2, 3, 4),
        scratch=(
            pltpu.VMEM((rank, rows), jnp.float32),
            pltpu.SemaphoreType.DMA((2 * (rows // CHUNK) + 2,)),
        ),
    )
    tiles = exchanged(packed, near_groups)

    share = f32(rank + EXTRA, 2 * half)

    def share_for(distance):
        kernel = functools.partial(share_kernel, distance=distance)
        return call(kernel, share, me, snaps_in, final_in, vectors_in, smem=1)

    two_right, left, one_right = share_for(2), share_for(3), share_for(1)
    from_left = sent(two_right, 1)

    copied = functools.partial(sum_and_copy_kernel, size=size)
    tiles = call(functools.partial(copied, copies=far), f32(far * size, LANES), tiles)
    tiles = exchanged(tiles, far_groups)
    from_left = sent(call(add_kernel, share, one_right, from_left), 1)
    from_right = sent(left, -1)

    tiles = call(functools.partial(copied, copies=near), f32(near * size, LANES), tiles)
    tiles = exchanged(tiles, near_groups)
    dmd_modes, last_rows = call(
        dmd_kernel,
        (f32(rank, 2 * half), f32(BLOCKS, rank)),
        me,
        snapshots,
        final_snapshot[None, :],
        right_vectors.T,
        from_right,
        from_left,
        sing,
        eigen_vectors,
        smem=1,
        hbm=(1, 2, 3),
        scratch=(
            pltpu.VMEM((2 * half, snapshots.shape[1]), jnp.float32),
            pltpu.VMEM((1, 2 * half), jnp.float32),
            pltpu.VMEM((rank, snapshots.shape[1]), jnp.float32),
            pltpu.SemaphoreType.DMA((3,)),
        ),
    )
    reduced_operator = call(operator_kernel, f32(rank, rank), tiles, last_rows, sing)
    return reduced_operator, dmd_modes.T


def solution(mesh):
    finer = Mesh(mesh.devices.reshape(4, 2, 4, 2, 2, mesh.shape["tm"]), (*SPACE, "tm"))
    return jax.shard_map(
        step,
        mesh=finer,
        in_specs=(P(SPACE, "tm"), P(SPACE), P(SPACE, None), P("tm", None), P(), P()),
        out_specs=(P(), P((*SPACE, "tm"), None)),
        check_vma=False,
    )
```

```python
import functools

import jax
import jax.numpy as jnp
import numpy as np
from jax import lax
from jax.experimental import pallas as pl
from jax.experimental.pallas import tpu as pltpu
from jax.sharding import Mesh
from jax.sharding import PartitionSpec as P

SPACE = ("y_far", "y_near", "z_far", "z_near", "core")
ALL = (*SPACE, "tm")
NEAR = ("y_near", "z_near", "core", "tm")
FAR = ("y_far", "z_far")
NEAR_FIRST = (1, 1, 1, 2)
FAR_FIRST = (2, 3)
LANES = 128
BLOCKS = 4
EXTRA = 2 * BLOCKS
CHUNK = 512
VMEM_GRANT = 16 << 20


def f32(*shape):
    return jax.ShapeDtypeStruct(shape, jnp.float32)


def call(kernel, out, *args, smem=0, hbm=(), scratch=()):
    whole = pl.BlockSpec(memory_space=pltpu.VMEM)
    scalar = pl.BlockSpec(memory_space=pltpu.SMEM)
    outs = out if isinstance(out, tuple) else (out,)
    specs = [scalar] * smem + [whole] * (len(args) - smem)
    args = list(args)
    for i in hbm:
        specs[i] = pl.BlockSpec(memory_space=pltpu.HBM)
        args[i] = pltpu.with_memory_space_constraint(args[i], pltpu.HBM)
    result = pl.pallas_call(
        kernel,
        out_shape=outs,
        in_specs=specs,
        scratch_shapes=scratch,
        out_specs=[whole] * len(outs),
        compiler_params=pltpu.CompilerParams(vmem_limit_bytes=VMEM_GRANT),
    )(*args)
    return result if isinstance(out, tuple) else result[0]


def split(x):
    high = x.astype(jnp.bfloat16)
    return high, (x - high.astype(jnp.float32)).astype(jnp.bfloat16)


def three_pass(a, b, contract=(1, 1)):
    dims = (((contract[0],), (contract[1],)), ((), ()))
    dot = functools.partial(
        lax.dot_general, dimension_numbers=dims, preferred_element_type=jnp.float32
    )
    (a_high, a_low), (b_high, b_low) = a, b
    return dot(a_high, b_high) + (dot(a_high, b_low) + dot(a_low, b_high))


def shifted(vectors):
    lane = lax.broadcasted_iota(jnp.int32, vectors.shape, 1)
    return jnp.where(lane == 0, 0.0, pltpu.roll(vectors, 1, 1))


def turned(row):
    row = jnp.pad(row, ((0, 0), (0, 2 * LANES - row.shape[1])))
    halves = [
        jnp.broadcast_to(row[:, i * LANES : (i + 1) * LANES], (LANES, LANES)).T[:, :1]
        for i in range(2)
    ]
    return jnp.concatenate(halves, axis=0)


def term_kernel(
    me, snaps, final, modes, vectors, packed, snaps_in, final_in, vectors_in, modes_in, sems
):
    rank, _ = vectors.shape
    chunks = snaps.shape[0] // CHUNK
    spans = [pl.ds(i * CHUNK, CHUNK) for i in range(chunks)]
    got_modes = [
        pltpu.make_async_copy(modes.at[:, here], modes_in.at[:, here], sems.at[i])
        for i, here in enumerate(spans)
    ]
    got_snaps = [
        pltpu.make_async_copy(snaps.at[here, :], snaps_in.at[here, :], sems.at[chunks + i])
        for i, here in enumerate(spans)
    ]
    got_final = pltpu.make_async_copy(final, final_in, sems.at[2 * chunks])
    got_vectors = pltpu.make_async_copy(vectors, vectors_in, sems.at[2 * chunks + 1])
    got_final.start()
    for i in range(chunks):
        got_modes[i].start()
        got_snaps[i].start()
    got_vectors.start()

    total = of_final = None
    got_final.wait()
    for i, here in enumerate(spans):
        got_modes[i].wait()
        got_snaps[i].wait()
        left, last = modes_in[:, here], final_in[:, here]
        product = three_pass(split(left), split(snaps_in[here, :]), (1, 0))
        total = product if total is None else total + product
        for j in range(0, CHUNK, LANES):
            column = left[:, j : j + LANES] * last[:, j : j + LANES]
            of_final = column if of_final is None else of_final + column
    got_vectors.wait()
    whole = three_pass(split(total), split(shifted(vectors_in[...])))
    of_final = jnp.sum(of_final, axis=1, keepdims=True)
    first = jnp.where(me[0] == 0, of_final, total[:, :1])
    packed[:rank, :] = whole[:, :LANES]
    rest = rank - LANES
    tail = jnp.pad(whole[:, LANES:], ((0, 0), (0, LANES - rest)))
    lane = lax.broadcasted_iota(jnp.int32, tail.shape, 1)
    tail = jnp.where(lane == rest + me[0], first, tail)
    tail = jnp.pad(tail, ((0, 2 * LANES - rank), (0, 0)))
    used = rest + BLOCKS
    for i in range(2):
        turn = tail[i * LANES : (i + 1) * LANES].T
        packed[rank + i * used : rank + (i + 1) * used, :] = turn[:used]


def shares_of(me, snaps, final, vectors):
    rank, snapshots = vectors.shape
    points = snaps.shape[0]
    row = lax.broadcasted_iota(jnp.int32, (EXTRA, snapshots), 0)
    column = lax.broadcasted_iota(jnp.int32, (EXTRA, snapshots), 1)
    unit = jnp.where((row == me) & (column == 0), 1.0, 0.0)
    left = split(jnp.concatenate([shifted(vectors), unit], axis=0))
    tail = jnp.pad(vectors[:, snapshots - LANES :], ((0, 2 * LANES - rank), (0, 0)))
    last = [tail[:LANES].T[LANES - 1 :], tail[LANES:].T[LANES - 1 :]]
    last = jnp.concatenate(last * (points // (2 * LANES)), axis=1)
    block = three_pass(left, split(snaps))
    slot = lax.broadcasted_iota(jnp.int32, (EXTRA, points), 0)
    extra = jnp.where((slot == me) & (me == 0), final, block[rank:])
    extra = jnp.where(slot == BLOCKS + lax.rem(me + 1, BLOCKS), last, extra)
    return block[:rank], extra


def share_kernel(me, snaps, final, vectors, out, *, distance):
    rank, points = vectors.shape[0], out.shape[1]
    owner = lax.rem(me[0] + distance, BLOCKS)
    here = pl.ds(pl.multiple_of(owner * points, points), points)
    out[:rank, :], out[rank:, :] = shares_of(me[0], snaps[here, :], final[:, here], vectors[...])


def add_kernel(own, arrived, out):
    out[...] = own[...] + arrived[...]


def sum_and_copy_kernel(tiles, out, *, size, copies):
    total = tiles[:size, :]
    for i in range(1, tiles.shape[0] // size):
        total = total + tiles[i * size : (i + 1) * size, :]
    for i in range(copies):
        out[i * size : (i + 1) * size, :] = total


def own_share_kernel(me, snaps, final, vectors, out, snaps_in, final_in, vectors_in, sems):
    rank, points = vectors.shape[0], out.shape[1]
    here = pl.ds(pl.multiple_of(me[0] * points, points), points)
    copies = (
        pltpu.make_async_copy(vectors, vectors_in, sems.at[0]),
        pltpu.make_async_copy(snaps.at[here, :], snaps_in, sems.at[1]),
        pltpu.make_async_copy(final.at[:, here], final_in, sems.at[2]),
    )
    for copy in copies:
        copy.start()
    for copy in copies:
        copy.wait()
    out[:rank, :], out[rank:, :] = shares_of(me[0], snaps_in[...], final_in[...], vectors_in[...])


def dmd_kernel(own, from_right, from_left, sing, eigen, out, rows):
    rank = out.shape[0]
    scale = turned(sing[...])[:rank]
    total = own[...] + from_right[...] + from_left[...]
    first = total[rank : rank + BLOCKS]
    last = total[rank + BLOCKS :, :rank]
    rows[...] = last
    summed = total[:rank] + three_pass(split(last), split(first), (0, 0))
    out[...] = three_pass(split(eigen[...]), split(summed * scale), (0, 0))


def operator_kernel(packed, rows, sing, out):
    rank = out.shape[0]
    rest = rank - LANES
    used = rest + BLOCKS
    first = jnp.concatenate(
        [
            packed[rank + rest : rank + used, :],
            packed[rank + used + rest : rank + 2 * used, :][:, :rest],
        ],
        axis=1,
    )
    term = three_pass(split(first), split(rows[...]), (0, 0))
    scale = sing[...]
    out[:, :LANES] = (packed[:rank, :] + term[:, :LANES]) * scale[:, :LANES]
    for i, size in ((0, LANES), (1, rest)):
        tail = packed[rank + i * used : rank + i * used + rest, :]
        turn = jnp.pad(tail, ((0, LANES - rest), (0, 0))).T[:size, :rest]
        here = slice(i * LANES, i * LANES + size)
        out[here, LANES:] = (turn + term[here, LANES:]) * scale[:, LANES:]


def groups_of(axes, first):
    sizes = {axis: lax.axis_size(axis) for axis in ALL}
    places = np.arange(np.prod(list(sizes.values()))).reshape(*sizes.values())
    for axis, start in zip(axes, first, strict=True):
        places = np.roll(places, -start, ALL.index(axis))
    others = [i for i, axis in enumerate(ALL) if axis not in axes]
    places = places.transpose(*others, *(ALL.index(axis) for axis in axes))
    return places.reshape(-1, int(np.prod([sizes[axis] for axis in axes]))).tolist()


def exchanged(tiles, groups):
    pieces = tiles.reshape(len(groups[0]), -1)
    got = lax.all_to_all(
        pieces, ALL, split_axis=0, concat_axis=0, tiled=True, axis_index_groups=groups
    )
    return got.reshape(tiles.shape)


def step(snapshots, final_snapshot, pod_modes, right_vectors, inverse_sing, eigen_vectors):
    blocks = lax.axis_size("tm")
    rows, rank = snapshots.shape[0], right_vectors.shape[1]
    half = rows // (2 * blocks)
    me = lax.axis_index("tm").astype(jnp.int32)[None]
    sing = inverse_sing[None, :]

    def sent(value, distance):
        return lax.ppermute(value, "tm", [(i, (i + distance) % blocks) for i in range(blocks)])

    near, far = lax.axis_size(NEAR), lax.axis_size(FAR)
    near_groups, far_groups = groups_of(NEAR, NEAR_FIRST), groups_of(FAR, FAR_FIRST)
    lines = rank + 2 * (rank - LANES + BLOCKS)
    size = lines // near
    packed, snaps_in, final_in, vectors_in = call(
        term_kernel,
        (
            f32(lines, LANES),
            pltpu.VMEM(snapshots.shape, jnp.float32),
            pltpu.VMEM((1, rows), jnp.float32),
            pltpu.VMEM((rank, snapshots.shape[1]), jnp.float32),
        ),
        me,
        snapshots,
        final_snapshot[None, :],
        pod_modes.T,
        right_vectors.T,
        smem=1,
        hbm=(1, 2, 3, 4),
        scratch=(
            pltpu.VMEM((rank, rows), jnp.float32),
            pltpu.SemaphoreType.DMA((2 * (rows // CHUNK) + 2,)),
        ),
    )
    tiles = exchanged(packed, near_groups)

    share = f32(rank + EXTRA, 2 * half)

    def share_for(distance):
        kernel = functools.partial(share_kernel, distance=distance)
        return call(kernel, share, me, snaps_in, final_in, vectors_in, smem=1)

    two_right, left, one_right = share_for(2), share_for(3), share_for(1)
    from_left = sent(two_right, 1)

    copied = functools.partial(sum_and_copy_kernel, size=size)
    tiles = call(functools.partial(copied, copies=far), f32(far * size, LANES), tiles)
    tiles = exchanged(tiles, far_groups)
    from_left = sent(call(add_kernel, share, one_right, from_left), 1)
    from_right = sent(left, -1)

    tiles = call(functools.partial(copied, copies=near), f32(near * size, LANES), tiles)
    tiles = exchanged(tiles, near_groups)
    own = call(
        own_share_kernel,
        share,
        me,
        snapshots,
        final_snapshot[None, :],
        right_vectors.T,
        smem=1,
        hbm=(1, 2, 3),
        scratch=(
            pltpu.VMEM((2 * half, snapshots.shape[1]), jnp.float32),
            pltpu.VMEM((1, 2 * half), jnp.float32),
            pltpu.VMEM((rank, snapshots.shape[1]), jnp.float32),
            pltpu.SemaphoreType.DMA((3,)),
        ),
    )
    dmd_modes, last_rows = call(
        dmd_kernel,
        (f32(rank, 2 * half), f32(BLOCKS, rank)),
        own,
        from_right,
        from_left,
        sing,
        eigen_vectors,
    )
    reduced_operator = call(operator_kernel, f32(rank, rank), tiles, last_rows, sing)
    return reduced_operator, dmd_modes.T


def solution(mesh):
    finer = Mesh(mesh.devices.reshape(4, 2, 4, 2, 2, mesh.shape["tm"]), (*SPACE, "tm"))
    return jax.shard_map(
        step,
        mesh=finer,
        in_specs=(P(SPACE, "tm"), P(SPACE), P(SPACE, None), P("tm", None), P(), P()),
        out_specs=(P(), P((*SPACE, "tm"), None)),
        check_vma=False,
    )
```

```python
import functools

import jax
import jax.numpy as jnp
import numpy as np
from jax import lax
from jax.experimental import pallas as pl
from jax.experimental.pallas import tpu as pltpu
from jax.sharding import Mesh
from jax.sharding import PartitionSpec as P

SPACE = ("y_far", "y_near", "z_far", "z_near", "core")
ALL = (*SPACE, "tm")
NEAR = ("y_near", "z_near", "core", "tm")
FAR = ("y_far", "z_far")
NEAR_FIRST = (1, 1, 1, 2)
FAR_FIRST = (2, 3)
LANES = 128
BLOCKS = 4
EXTRA = 2 * BLOCKS
VMEM_GRANT = 16 << 20


def f32(*shape):
    return jax.ShapeDtypeStruct(shape, jnp.float32)


def call(kernel, out, *args, smem=0, hbm=(), scratch=()):
    whole = pl.BlockSpec(memory_space=pltpu.VMEM)
    scalar = pl.BlockSpec(memory_space=pltpu.SMEM)
    outs = out if isinstance(out, tuple) else (out,)
    specs = [scalar] * smem + [whole] * (len(args) - smem)
    args = list(args)
    for i in hbm:
        specs[i] = pl.BlockSpec(memory_space=pltpu.HBM)
        args[i] = pltpu.with_memory_space_constraint(args[i], pltpu.HBM)
    result = pl.pallas_call(
        kernel,
        out_shape=outs,
        in_specs=specs,
        scratch_shapes=scratch,
        out_specs=[whole] * len(outs),
        compiler_params=pltpu.CompilerParams(vmem_limit_bytes=VMEM_GRANT),
    )(*args)
    return result if isinstance(out, tuple) else result[0]


def split(x):
    high = x.astype(jnp.bfloat16)
    return high, (x - high.astype(jnp.float32)).astype(jnp.bfloat16)


def three_pass(a, b, contract=(1, 1)):
    dims = (((contract[0],), (contract[1],)), ((), ()))
    dot = functools.partial(
        lax.dot_general, dimension_numbers=dims, preferred_element_type=jnp.float32
    )
    (a_high, a_low), (b_high, b_low) = a, b
    return dot(a_high, b_high) + (dot(a_high, b_low) + dot(a_low, b_high))


def shifted(vectors):
    lane = lax.broadcasted_iota(jnp.int32, vectors.shape, 1)
    return jnp.where(lane == 0, 0.0, pltpu.roll(vectors, 1, 1))


def turned(row):
    row = jnp.pad(row, ((0, 0), (0, 2 * LANES - row.shape[1])))
    halves = [
        jnp.broadcast_to(row[:, i * LANES : (i + 1) * LANES], (LANES, LANES)).T[:, :1]
        for i in range(2)
    ]
    return jnp.concatenate(halves, axis=0)


def term_kernel(
    me, snaps, final, modes, vectors, packed, first_in, second_in, third_in, final_in, vectors_in, own_in, modes_in, sems
):
    rank, _ = vectors.shape
    points = own_in.shape[0]
    held = (own_in, first_in, second_in, third_in)
    spans = [
        pl.ds(pl.multiple_of(lax.rem(me[0] + i, BLOCKS) * points, points), points)
        for i in range(BLOCKS)
    ]
    got_modes = [
        pltpu.make_async_copy(modes.at[:, here], modes_in.at[:, pl.ds(i * points, points)], sems.at[i])
        for i, here in enumerate(spans)
    ]
    got_snaps = [
        pltpu.make_async_copy(snaps.at[here, :], held[i], sems.at[BLOCKS + i])
        for i, here in enumerate(spans)
    ]
    got_final = pltpu.make_async_copy(final, final_in, sems.at[2 * BLOCKS])
    got_vectors = pltpu.make_async_copy(vectors, vectors_in, sems.at[2 * BLOCKS + 1])
    got_final.start()
    for i in range(BLOCKS):
        got_modes[i].start()
        got_snaps[i].start()
    got_vectors.start()

    total = of_final = None
    got_final.wait()
    for i, here in enumerate(spans):
        got_modes[i].wait()
        got_snaps[i].wait()
        left, last = modes_in[:, i * points : (i + 1) * points], final_in[:, here]
        product = three_pass(split(left), split(held[i][...]), (1, 0))
        total = product if total is None else total + product
        for j in range(0, points, LANES):
            column = left[:, j : j + LANES] * last[:, j : j + LANES]
            of_final = column if of_final is None else of_final + column
    got_vectors.wait()
    whole = three_pass(split(total), split(shifted(vectors_in[...])))
    of_final = jnp.sum(of_final, axis=1, keepdims=True)
    first = jnp.where(me[0] == 0, of_final, total[:, :1])
    packed[:rank, :] = whole[:, :LANES]
    rest = rank - LANES
    tail = jnp.pad(whole[:, LANES:], ((0, 0), (0, LANES - rest)))
    lane = lax.broadcasted_iota(jnp.int32, tail.shape, 1)
    tail = jnp.where(lane == rest + me[0], first, tail)
    tail = jnp.pad(tail, ((0, 2 * LANES - rank), (0, 0)))
    used = rest + BLOCKS
    for i in range(2):
        turn = tail[i * LANES : (i + 1) * LANES].T
        packed[rank + i * used : rank + (i + 1) * used, :] = turn[:used]


def shares_of(me, snaps, final, vectors):
    rank, snapshots = vectors.shape
    points = snaps.shape[0]
    row = lax.broadcasted_iota(jnp.int32, (EXTRA, snapshots), 0)
    column = lax.broadcasted_iota(jnp.int32, (EXTRA, snapshots), 1)
    unit = jnp.where((row == me) & (column == 0), 1.0, 0.0)
    left = split(jnp.concatenate([shifted(vectors), unit], axis=0))
    tail = jnp.pad(vectors[:, snapshots - LANES :], ((0, 2 * LANES - rank), (0, 0)))
    last = [tail[:LANES].T[LANES - 1 :], tail[LANES:].T[LANES - 1 :]]
    last = jnp.concatenate(last * (points // (2 * LANES)), axis=1)
    block = three_pass(left, split(snaps))
    slot = lax.broadcasted_iota(jnp.int32, (EXTRA, points), 0)
    extra = jnp.where((slot == me) & (me == 0), final, block[rank:])
    extra = jnp.where(slot == BLOCKS + lax.rem(me + 1, BLOCKS), last, extra)
    return block[:rank], extra


def share_kernel(me, snaps, final, vectors, out, *, distance):
    rank, points = vectors.shape[0], out.shape[1]
    owner = lax.rem(me[0] + distance, BLOCKS)
    here = pl.ds(pl.multiple_of(owner * points, points), points)
    out[:rank, :], out[rank:, :] = shares_of(me[0], snaps[...], final[:, here], vectors[...])


def add_kernel(own, arrived, out):
    out[...] = own[...] + arrived[...]


def sum_and_copy_kernel(tiles, out, *, size, copies):
    total = tiles[:size, :]
    for i in range(1, tiles.shape[0] // size):
        total = total + tiles[i * size : (i + 1) * size, :]
    for i in range(copies):
        out[i * size : (i + 1) * size, :] = total


def own_share_kernel(me, snaps, final, vectors, out, snaps_in, final_in, vectors_in, sems):
    rank, points = vectors.shape[0], out.shape[1]
    here = pl.ds(pl.multiple_of(me[0] * points, points), points)
    copies = (
        pltpu.make_async_copy(vectors, vectors_in, sems.at[0]),
        pltpu.make_async_copy(snaps.at[here, :], snaps_in, sems.at[1]),
        pltpu.make_async_copy(final.at[:, here], final_in, sems.at[2]),
    )
    for copy in copies:
        copy.start()
    for copy in copies:
        copy.wait()
    out[:rank, :], out[rank:, :] = shares_of(me[0], snaps_in[...], final_in[...], vectors_in[...])


def dmd_kernel(own, from_right, from_left, sing, eigen, out, rows):
    rank = out.shape[0]
    scale = turned(sing[...])[:rank]
    total = own[...] + from_right[...] + from_left[...]
    first = total[rank : rank + BLOCKS]
    last = total[rank + BLOCKS :, :rank]
    rows[...] = last
    summed = total[:rank] + three_pass(split(last), split(first), (0, 0))
    out[...] = three_pass(split(eigen[...]), split(summed * scale), (0, 0))


def operator_kernel(packed, rows, sing, out):
    rank = out.shape[0]
    rest = rank - LANES
    used = rest + BLOCKS
    first = jnp.concatenate(
        [
            packed[rank + rest : rank + used, :],
            packed[rank + used + rest : rank + 2 * used, :][:, :rest],
        ],
        axis=1,
    )
    term = three_pass(split(first), split(rows[...]), (0, 0))
    scale = sing[...]
    out[:, :LANES] = (packed[:rank, :] + term[:, :LANES]) * scale[:, :LANES]
    for i, size in ((0, LANES), (1, rest)):
        tail = packed[rank + i * used : rank + i * used + rest, :]
        turn = jnp.pad(tail, ((0, LANES - rest), (0, 0))).T[:size, :rest]
        here = slice(i * LANES, i * LANES + size)
        out[here, LANES:] = (turn + term[here, LANES:]) * scale[:, LANES:]


def groups_of(axes, first):
    sizes = {axis: lax.axis_size(axis) for axis in ALL}
    places = np.arange(np.prod(list(sizes.values()))).reshape(*sizes.values())
    for axis, start in zip(axes, first, strict=True):
        places = np.roll(places, -start, ALL.index(axis))
    others = [i for i, axis in enumerate(ALL) if axis not in axes]
    places = places.transpose(*others, *(ALL.index(axis) for axis in axes))
    return places.reshape(-1, int(np.prod([sizes[axis] for axis in axes]))).tolist()


def exchanged(tiles, groups):
    pieces = tiles.reshape(len(groups[0]), -1)
    got = lax.all_to_all(
        pieces, ALL, split_axis=0, concat_axis=0, tiled=True, axis_index_groups=groups
    )
    return got.reshape(tiles.shape)


def step(snapshots, final_snapshot, pod_modes, right_vectors, inverse_sing, eigen_vectors):
    blocks = lax.axis_size("tm")
    rows, rank = snapshots.shape[0], right_vectors.shape[1]
    half = rows // (2 * blocks)
    me = lax.axis_index("tm").astype(jnp.int32)[None]
    sing = inverse_sing[None, :]

    def sent(value, distance):
        return lax.ppermute(value, "tm", [(i, (i + distance) % blocks) for i in range(blocks)])

    near, far = lax.axis_size(NEAR), lax.axis_size(FAR)
    near_groups, far_groups = groups_of(NEAR, NEAR_FIRST), groups_of(FAR, FAR_FIRST)
    lines = rank + 2 * (rank - LANES + BLOCKS)
    size = lines // near
    packed, *snaps_in, final_in, vectors_in = call(
        term_kernel,
        (
            f32(lines, LANES),
            *[f32(2 * half, snapshots.shape[1])] * (BLOCKS - 1),
            f32(1, rows),
            f32(rank, snapshots.shape[1]),
        ),
        me,
        snapshots,
        final_snapshot[None, :],
        pod_modes.T,
        right_vectors.T,
        smem=1,
        hbm=(1, 2, 3, 4),
        scratch=(
            pltpu.VMEM((2 * half, snapshots.shape[1]), jnp.float32),
            pltpu.VMEM((rank, rows), jnp.float32),
            pltpu.SemaphoreType.DMA((2 * BLOCKS + 2,)),
        ),
    )
    tiles = exchanged(packed, near_groups)

    share = f32(rank + EXTRA, 2 * half)

    def share_for(distance):
        kernel = functools.partial(share_kernel, distance=distance)
        return call(kernel, share, me, snaps_in[distance - 1], final_in, vectors_in, smem=1)

    two_right, left, one_right = share_for(2), share_for(3), share_for(1)
    from_left = sent(two_right, 1)

    copied = functools.partial(sum_and_copy_kernel, size=size)
    tiles = call(functools.partial(copied, copies=far), f32(far * size, LANES), tiles)
    tiles = exchanged(tiles, far_groups)
    from_left = sent(call(add_kernel, share, one_right, from_left), 1)
    from_right = sent(left, -1)

    tiles = call(functools.partial(copied, copies=near), f32(near * size, LANES), tiles)
    tiles = exchanged(tiles, near_groups)
    own = call(
        own_share_kernel,
        share,
        me,
        snapshots,
        final_snapshot[None, :],
        right_vectors.T,
        smem=1,
        hbm=(1, 2, 3),
        scratch=(
            pltpu.VMEM((2 * half, snapshots.shape[1]), jnp.float32),
            pltpu.VMEM((1, 2 * half), jnp.float32),
            pltpu.VMEM((rank, snapshots.shape[1]), jnp.float32),
            pltpu.SemaphoreType.DMA((3,)),
        ),
    )
    dmd_modes, last_rows = call(
        dmd_kernel,
        (f32(rank, 2 * half), f32(BLOCKS, rank)),
        own,
        from_right,
        from_left,
        sing,
        eigen_vectors,
    )
    reduced_operator = call(operator_kernel, f32(rank, rank), tiles, last_rows, sing)
    return reduced_operator, dmd_modes.T


def solution(mesh):
    finer = Mesh(mesh.devices.reshape(4, 2, 4, 2, 2, mesh.shape["tm"]), (*SPACE, "tm"))
    return jax.shard_map(
        step,
        mesh=finer,
        in_specs=(P(SPACE, "tm"), P(SPACE), P(SPACE, None), P("tm", None), P(), P()),
        out_specs=(P(), P((*SPACE, "tm"), None)),
        check_vma=False,
    )
```

```python
import functools

import jax
import jax.numpy as jnp
import numpy as np
from jax import lax
from jax.experimental import pallas as pl
from jax.experimental.pallas import tpu as pltpu
from jax.sharding import Mesh
from jax.sharding import PartitionSpec as P

SPACE = ("y_far", "y_near", "z_far", "z_near", "core")
ALL = (*SPACE, "tm")
NEAR = ("y_near", "z_near", "core", "tm")
FAR = ("y_far", "z_far")
NEAR_FIRST = (1, 1, 1, 2)
FAR_FIRST = (2, 3)
LANES = 128
BLOCKS = 4
EXTRA = 2 * BLOCKS
VMEM_GRANT = 16 << 20


def f32(*shape):
    return jax.ShapeDtypeStruct(shape, jnp.float32)


def call(kernel, out, *args, smem=0, hbm=(), scratch=()):
    whole = pl.BlockSpec(memory_space=pltpu.VMEM)
    scalar = pl.BlockSpec(memory_space=pltpu.SMEM)
    outs = out if isinstance(out, tuple) else (out,)
    specs = [scalar] * smem + [whole] * (len(args) - smem)
    args = list(args)
    for i in hbm:
        specs[i] = pl.BlockSpec(memory_space=pltpu.HBM)
        args[i] = pltpu.with_memory_space_constraint(args[i], pltpu.HBM)
    result = pl.pallas_call(
        kernel,
        out_shape=outs,
        in_specs=specs,
        scratch_shapes=scratch,
        out_specs=[whole] * len(outs),
        compiler_params=pltpu.CompilerParams(vmem_limit_bytes=VMEM_GRANT),
    )(*args)
    return result if isinstance(out, tuple) else result[0]


def split(x):
    high = x.astype(jnp.bfloat16)
    return high, (x - high.astype(jnp.float32)).astype(jnp.bfloat16)


def three_pass(a, b, contract=(1, 1)):
    dims = (((contract[0],), (contract[1],)), ((), ()))
    dot = functools.partial(
        lax.dot_general, dimension_numbers=dims, preferred_element_type=jnp.float32
    )
    (a_high, a_low), (b_high, b_low) = a, b
    return dot(a_high, b_high) + (dot(a_high, b_low) + dot(a_low, b_high))


def block_and_step(place):
    return lax.rem(place, BLOCKS), 1 + (BLOCKS - 2) * lax.div(place, BLOCKS)


def shifted(vectors):
    lane = lax.broadcasted_iota(jnp.int32, vectors.shape, 1)
    return jnp.where(lane == 0, 0.0, pltpu.roll(vectors, 1, 1))


def turned(row):
    row = jnp.pad(row, ((0, 0), (0, 2 * LANES - row.shape[1])))
    halves = [
        jnp.broadcast_to(row[:, i * LANES : (i + 1) * LANES], (LANES, LANES)).T[:, :1]
        for i in range(2)
    ]
    return jnp.concatenate(halves, axis=0)


def term_kernel(
    place, snaps, final, modes, vectors, packed, first_in, second_in, third_in, final_in, vectors_in, own_in, modes_in, sems
):
    rank, _ = vectors.shape
    points = own_in.shape[0]
    block, step = block_and_step(place[0])
    held = (own_in, first_in, second_in, third_in)
    spans = [
        pl.ds(pl.multiple_of(lax.rem(block + i * step, BLOCKS) * points, points), points)
        for i in range(BLOCKS)
    ]
    got_modes = [
        pltpu.make_async_copy(modes.at[:, here], modes_in.at[:, pl.ds(i * points, points)], sems.at[i])
        for i, here in enumerate(spans)
    ]
    got_snaps = [
        pltpu.make_async_copy(snaps.at[here, :], held[i], sems.at[BLOCKS + i])
        for i, here in enumerate(spans)
    ]
    got_final = pltpu.make_async_copy(final, final_in, sems.at[2 * BLOCKS])
    got_vectors = pltpu.make_async_copy(vectors, vectors_in, sems.at[2 * BLOCKS + 1])
    got_final.start()
    for i in range(BLOCKS):
        got_modes[i].start()
        got_snaps[i].start()
    got_vectors.start()

    total = of_final = None
    got_final.wait()
    for i, here in enumerate(spans):
        got_modes[i].wait()
        got_snaps[i].wait()
        left, last = modes_in[:, i * points : (i + 1) * points], final_in[:, here]
        product = three_pass(split(left), split(held[i][...]), (1, 0))
        total = product if total is None else total + product
        for j in range(0, points, LANES):
            column = left[:, j : j + LANES] * last[:, j : j + LANES]
            of_final = column if of_final is None else of_final + column
    got_vectors.wait()
    whole = three_pass(split(total), split(shifted(vectors_in[...])))
    of_final = jnp.sum(of_final, axis=1, keepdims=True)
    first = jnp.where(block == 0, of_final, total[:, :1])
    packed[:rank, :] = whole[:, :LANES]
    rest = rank - LANES
    tail = jnp.pad(whole[:, LANES:], ((0, 0), (0, LANES - rest)))
    lane = lax.broadcasted_iota(jnp.int32, tail.shape, 1)
    tail = jnp.where(lane == rest + block, first, tail)
    tail = jnp.pad(tail, ((0, 2 * LANES - rank), (0, 0)))
    used = rest + BLOCKS
    for i in range(2):
        turn = tail[i * LANES : (i + 1) * LANES].T
        packed[rank + i * used : rank + (i + 1) * used, :] = turn[:used]


def shares_of(me, snaps, final, vectors):
    rank, snapshots = vectors.shape
    points = snaps.shape[0]
    row = lax.broadcasted_iota(jnp.int32, (EXTRA, snapshots), 0)
    column = lax.broadcasted_iota(jnp.int32, (EXTRA, snapshots), 1)
    unit = jnp.where((row == me) & (column == 0), 1.0, 0.0)
    left = split(jnp.concatenate([shifted(vectors), unit], axis=0))
    tail = jnp.pad(vectors[:, snapshots - LANES :], ((0, 2 * LANES - rank), (0, 0)))
    last = [tail[:LANES].T[LANES - 1 :], tail[LANES:].T[LANES - 1 :]]
    last = jnp.concatenate(last * (points // (2 * LANES)), axis=1)
    block = three_pass(left, split(snaps))
    slot = lax.broadcasted_iota(jnp.int32, (EXTRA, points), 0)
    extra = jnp.where((slot == me) & (me == 0), final, block[rank:])
    extra = jnp.where(slot == BLOCKS + lax.rem(me + 1, BLOCKS), last, extra)
    return block[:rank], extra


def share_kernel(place, snaps, final, vectors, out, *, distance):
    rank, points = vectors.shape[0], out.shape[1]
    block, step = block_and_step(place[0])
    owner = lax.rem(block + distance * step, BLOCKS)
    here = pl.ds(pl.multiple_of(owner * points, points), points)
    out[:rank, :], out[rank:, :] = shares_of(block, snaps[...], final[:, here], vectors[...])


def add_kernel(own, arrived, out):
    out[...] = own[...] + arrived[...]


def sum_and_copy_kernel(tiles, out, *, size, copies):
    total = tiles[:size, :]
    for i in range(1, tiles.shape[0] // size):
        total = total + tiles[i * size : (i + 1) * size, :]
    for i in range(copies):
        out[i * size : (i + 1) * size, :] = total


def own_share_kernel(place, snaps, final, vectors, out, snaps_in, final_in, vectors_in, sems):
    rank, points = vectors.shape[0], out.shape[1]
    block, _ = block_and_step(place[0])
    here = pl.ds(pl.multiple_of(block * points, points), points)
    copies = (
        pltpu.make_async_copy(vectors, vectors_in, sems.at[0]),
        pltpu.make_async_copy(snaps.at[here, :], snaps_in, sems.at[1]),
        pltpu.make_async_copy(final.at[:, here], final_in, sems.at[2]),
    )
    for copy in copies:
        copy.start()
    for copy in copies:
        copy.wait()
    out[:rank, :], out[rank:, :] = shares_of(block, snaps_in[...], final_in[...], vectors_in[...])


def dmd_kernel(own, from_right, from_left, sing, eigen, out, rows):
    rank = out.shape[0]
    scale = turned(sing[...])[:rank]
    total = own[...] + from_right[...] + from_left[...]
    first = total[rank : rank + BLOCKS]
    last = total[rank + BLOCKS :, :rank]
    rows[...] = last
    summed = total[:rank] + three_pass(split(last), split(first), (0, 0))
    out[...] = three_pass(split(eigen[...]), split(summed * scale), (0, 0))


def operator_kernel(packed, rows, sing, out):
    rank = out.shape[0]
    rest = rank - LANES
    used = rest + BLOCKS
    first = jnp.concatenate(
        [
            packed[rank + rest : rank + used, :],
            packed[rank + used + rest : rank + 2 * used, :][:, :rest],
        ],
        axis=1,
    )
    term = three_pass(split(first), split(rows[...]), (0, 0))
    scale = sing[...]
    out[:, :LANES] = (packed[:rank, :] + term[:, :LANES]) * scale[:, :LANES]
    for i, size in ((0, LANES), (1, rest)):
        tail = packed[rank + i * used : rank + i * used + rest, :]
        turn = jnp.pad(tail, ((0, LANES - rest), (0, 0))).T[:size, :rest]
        here = slice(i * LANES, i * LANES + size)
        out[here, LANES:] = (turn + term[here, LANES:]) * scale[:, LANES:]


def groups_of(axes, first):
    sizes = {axis: lax.axis_size(axis) for axis in ALL}
    places = np.arange(np.prod(list(sizes.values()))).reshape(*sizes.values())
    for axis, start in zip(axes, first, strict=True):
        places = np.roll(places, -start, ALL.index(axis))
    others = [i for i, axis in enumerate(ALL) if axis not in axes]
    places = places.transpose(*others, *(ALL.index(axis) for axis in axes))
    return places.reshape(-1, int(np.prod([sizes[axis] for axis in axes]))).tolist()


def exchanged(tiles, groups):
    pieces = tiles.reshape(len(groups[0]), -1)
    got = lax.all_to_all(
        pieces, ALL, split_axis=0, concat_axis=0, tiled=True, axis_index_groups=groups
    )
    return got.reshape(tiles.shape)


def step(snapshots, final_snapshot, pod_modes, right_vectors, inverse_sing, eigen_vectors):
    blocks = lax.axis_size("tm")
    rows, rank = snapshots.shape[0], right_vectors.shape[1]
    half = rows // (2 * blocks)
    place = lax.axis_index(("core", "tm")).astype(jnp.int32)[None]
    sing = inverse_sing[None, :]

    def sent(value, distance):
        return lax.ppermute(
            value,
            ("core", "tm"),
            [
                (core * blocks + i, core * blocks + (i + distance * (1 - 2 * core)) % blocks)
                for core in range(lax.axis_size("core"))
                for i in range(blocks)
            ],
        )

    near, far = lax.axis_size(NEAR), lax.axis_size(FAR)
    near_groups, far_groups = groups_of(NEAR, NEAR_FIRST), groups_of(FAR, FAR_FIRST)
    lines = rank + 2 * (rank - LANES + BLOCKS)
    size = lines // near
    packed, *snaps_in, final_in, vectors_in = call(
        term_kernel,
        (
            f32(lines, LANES),
            *[f32(2 * half, snapshots.shape[1])] * (BLOCKS - 1),
            f32(1, rows),
            f32(rank, snapshots.shape[1]),
        ),
        place,
        snapshots,
        final_snapshot[None, :],
        pod_modes.T,
        right_vectors.T,
        smem=1,
        hbm=(1, 2, 3, 4),
        scratch=(
            pltpu.VMEM((2 * half, snapshots.shape[1]), jnp.float32),
            pltpu.VMEM((rank, rows), jnp.float32),
            pltpu.SemaphoreType.DMA((2 * BLOCKS + 2,)),
        ),
    )
    tiles = exchanged(packed, near_groups)

    share = f32(rank + EXTRA, 2 * half)

    def share_for(distance):
        kernel = functools.partial(share_kernel, distance=distance)
        return call(kernel, share, place, snaps_in[distance - 1], final_in, vectors_in, smem=1)

    two_right, left, one_right = share_for(2), share_for(3), share_for(1)
    from_left = sent(two_right, 1)

    copied = functools.partial(sum_and_copy_kernel, size=size)
    tiles = call(functools.partial(copied, copies=far), f32(far * size, LANES), tiles)
    tiles = exchanged(tiles, far_groups)
    from_left = sent(call(add_kernel, share, one_right, from_left), 1)
    from_right = sent(left, -1)

    tiles = call(functools.partial(copied, copies=near), f32(near * size, LANES), tiles)
    tiles = exchanged(tiles, near_groups)
    own = call(
        own_share_kernel,
        share,
        place,
        snapshots,
        final_snapshot[None, :],
        right_vectors.T,
        smem=1,
        hbm=(1, 2, 3),
        scratch=(
            pltpu.VMEM((2 * half, snapshots.shape[1]), jnp.float32),
            pltpu.VMEM((1, 2 * half), jnp.float32),
            pltpu.VMEM((rank, snapshots.shape[1]), jnp.float32),
            pltpu.SemaphoreType.DMA((3,)),
        ),
    )
    dmd_modes, last_rows = call(
        dmd_kernel,
        (f32(rank, 2 * half), f32(BLOCKS, rank)),
        own,
        from_right,
        from_left,
        sing,
        eigen_vectors,
    )
    reduced_operator = call(operator_kernel, f32(rank, rank), tiles, last_rows, sing)
    return reduced_operator, dmd_modes.T


def solution(mesh):
    finer = Mesh(mesh.devices.reshape(4, 2, 4, 2, 2, mesh.shape["tm"]), (*SPACE, "tm"))
    return jax.shard_map(
        step,
        mesh=finer,
        in_specs=(P(SPACE, "tm"), P(SPACE), P(SPACE, None), P("tm", None), P(), P()),
        out_specs=(P(), P((*SPACE, "tm"), None)),
        check_vma=False,
    )
```

```python
import functools

import jax
import jax.numpy as jnp
import numpy as np
from jax import lax
from jax.experimental import pallas as pl
from jax.experimental.pallas import tpu as pltpu
from jax.sharding import Mesh
from jax.sharding import PartitionSpec as P

SPACE = ("y_far", "y_near", "z_far", "z_near", "core")
ALL = (*SPACE, "tm")
NEAR = ("y_near", "z_near", "core", "tm")
FAR = ("y_far", "z_far")
NEAR_FIRST = (0, 1, 1, 2)
FAR_FIRST = (3, 3)
LANES = 128
BLOCKS = 4
EXTRA = 2 * BLOCKS
VMEM_GRANT = 16 << 20


def f32(*shape):
    return jax.ShapeDtypeStruct(shape, jnp.float32)


def call(kernel, out, *args, smem=0, hbm=(), scratch=()):
    whole = pl.BlockSpec(memory_space=pltpu.VMEM)
    scalar = pl.BlockSpec(memory_space=pltpu.SMEM)
    outs = out if isinstance(out, tuple) else (out,)
    specs = [scalar] * smem + [whole] * (len(args) - smem)
    args = list(args)
    for i in hbm:
        specs[i] = pl.BlockSpec(memory_space=pltpu.HBM)
        args[i] = pltpu.with_memory_space_constraint(args[i], pltpu.HBM)
    result = pl.pallas_call(
        kernel,
        out_shape=outs,
        in_specs=specs,
        scratch_shapes=scratch,
        out_specs=[whole] * len(outs),
        compiler_params=pltpu.CompilerParams(vmem_limit_bytes=VMEM_GRANT),
    )(*args)
    return result if isinstance(out, tuple) else result[0]


def split(x):
    high = x.astype(jnp.bfloat16)
    return high, (x - high.astype(jnp.float32)).astype(jnp.bfloat16)


def three_pass(a, b, contract=(1, 1)):
    dims = (((contract[0],), (contract[1],)), ((), ()))
    dot = functools.partial(
        lax.dot_general, dimension_numbers=dims, preferred_element_type=jnp.float32
    )
    (a_high, a_low), (b_high, b_low) = a, b
    return dot(a_high, b_high) + (dot(a_high, b_low) + dot(a_low, b_high))


def block_and_step(place):
    return lax.rem(place, BLOCKS), 1 + (BLOCKS - 2) * lax.div(place, BLOCKS)


def shifted(vectors):
    lane = lax.broadcasted_iota(jnp.int32, vectors.shape, 1)
    return jnp.where(lane == 0, 0.0, pltpu.roll(vectors, 1, 1))


def turned(row):
    row = jnp.pad(row, ((0, 0), (0, 2 * LANES - row.shape[1])))
    halves = [
        jnp.broadcast_to(row[:, i * LANES : (i + 1) * LANES], (LANES, LANES)).T[:, :1]
        for i in range(2)
    ]
    return jnp.concatenate(halves, axis=0)


def term_kernel(
    place, snaps, final, modes, vectors, packed, first_in, second_in, third_in, final_in, vectors_in, own_in, modes_in, sems
):
    rank, _ = vectors.shape
    points = own_in.shape[0]
    block, step = block_and_step(place[0])
    held = (own_in, first_in, second_in, third_in)
    spans = [
        pl.ds(pl.multiple_of(lax.rem(block + i * step, BLOCKS) * points, points), points)
        for i in range(BLOCKS)
    ]
    got_modes = [
        pltpu.make_async_copy(modes.at[:, here], modes_in.at[:, pl.ds(i * points, points)], sems.at[i])
        for i, here in enumerate(spans)
    ]
    got_snaps = [
        pltpu.make_async_copy(snaps.at[here, :], held[i], sems.at[BLOCKS + i])
        for i, here in enumerate(spans)
    ]
    got_final = pltpu.make_async_copy(final, final_in, sems.at[2 * BLOCKS])
    got_vectors = pltpu.make_async_copy(vectors, vectors_in, sems.at[2 * BLOCKS + 1])
    got_vectors.start()
    got_final.start()
    for i in range(BLOCKS):
        got_modes[i].start()
        got_snaps[i].start()

    total = of_final = None
    got_vectors.wait()
    right = split(shifted(vectors_in[...]))
    got_final.wait()
    for i, here in enumerate(spans):
        got_modes[i].wait()
        got_snaps[i].wait()
        left, last = modes_in[:, i * points : (i + 1) * points], final_in[:, here]
        product = three_pass(split(left), split(held[i][...]), (1, 0))
        total = product if total is None else total + product
        for j in range(0, points, LANES):
            column = left[:, j : j + LANES] * last[:, j : j + LANES]
            of_final = column if of_final is None else of_final + column
    whole = three_pass(split(total), right)
    of_final = jnp.sum(of_final, axis=1, keepdims=True)
    first = jnp.where(block == 0, of_final, total[:, :1])
    packed[:rank, :] = whole[:, :LANES]
    rest = rank - LANES
    tail = jnp.pad(whole[:, LANES:], ((0, 0), (0, LANES - rest)))
    lane = lax.broadcasted_iota(jnp.int32, tail.shape, 1)
    tail = jnp.where(lane == rest + block, first, tail)
    tail = jnp.pad(tail, ((0, 2 * LANES - rank), (0, 0)))
    used = rest + BLOCKS
    for i in range(2):
        turn = tail[i * LANES : (i + 1) * LANES].T
        packed[rank + i * used : rank + (i + 1) * used, :] = turn[:used]


def shares_of(me, snaps, final, vectors):
    rank, snapshots = vectors.shape
    points = snaps.shape[0]
    row = lax.broadcasted_iota(jnp.int32, (EXTRA, snapshots), 0)
    column = lax.broadcasted_iota(jnp.int32, (EXTRA, snapshots), 1)
    unit = jnp.where((row == me) & (column == 0), 1.0, 0.0)
    left = split(jnp.concatenate([shifted(vectors), unit], axis=0))
    tail = jnp.pad(vectors[:, snapshots - LANES :], ((0, 2 * LANES - rank), (0, 0)))
    last = [tail[:LANES].T[LANES - 1 :], tail[LANES:].T[LANES - 1 :]]
    last = jnp.concatenate(last * (points // (2 * LANES)), axis=1)
    block = three_pass(left, split(snaps))
    slot = lax.broadcasted_iota(jnp.int32, (EXTRA, points), 0)
    extra = jnp.where((slot == me) & (me == 0), final, block[rank:])
    extra = jnp.where(slot == BLOCKS + lax.rem(me + 1, BLOCKS), last, extra)
    return block[:rank], extra


def share_kernel(place, snaps, final, vectors, out, *, distance):
    rank, points = vectors.shape[0], out.shape[1]
    block, step = block_and_step(place[0])
    owner = lax.rem(block + distance * step, BLOCKS)
    here = pl.ds(pl.multiple_of(owner * points, points), points)
    out[:rank, :], out[rank:, :] = shares_of(block, snaps[...], final[:, here], vectors[...])


def add_kernel(own, arrived, out):
    out[...] = own[...] + arrived[...]


def sum_and_copy_kernel(tiles, out, *, size, copies):
    total = tiles[:size, :]
    for i in range(1, tiles.shape[0] // size):
        total = total + tiles[i * size : (i + 1) * size, :]
    for i in range(copies):
        out[i * size : (i + 1) * size, :] = total


def own_share_kernel(place, snaps, final, vectors, out, snaps_in, final_in, vectors_in, sems):
    rank, points = vectors.shape[0], out.shape[1]
    block, _ = block_and_step(place[0])
    here = pl.ds(pl.multiple_of(block * points, points), points)
    copies = (
        pltpu.make_async_copy(vectors, vectors_in, sems.at[0]),
        pltpu.make_async_copy(snaps.at[here, :], snaps_in, sems.at[1]),
        pltpu.make_async_copy(final.at[:, here], final_in, sems.at[2]),
    )
    for copy in copies:
        copy.start()
    for copy in copies:
        copy.wait()
    out[:rank, :], out[rank:, :] = shares_of(block, snaps_in[...], final_in[...], vectors_in[...])


def dmd_kernel(own, from_right, from_left, sing, eigen, out, rows):
    rank = out.shape[0]
    scale = turned(sing[...])[:rank]
    total = own[...] + from_right[...] + from_left[...]
    first = total[rank : rank + BLOCKS]
    last = total[rank + BLOCKS :, :rank]
    rows[...] = last
    summed = total[:rank] + three_pass(split(last), split(first), (0, 0))
    out[...] = three_pass(split(eigen[...]), split(summed * scale), (0, 0))


def operator_kernel(packed, rows, sing, out):
    rank = out.shape[0]
    rest = rank - LANES
    used = rest + BLOCKS
    scale = sing[...]
    for i, size in ((0, LANES), (1, rest)):
        tail = packed[rank + i * used : rank + (i + 1) * used, :]
        turn = jnp.pad(tail, ((0, LANES - used), (0, 0))).T[:size]
        term = turn[:, rest : rest + 1] * rows[:1, :]
        for j in range(1, BLOCKS):
            term = term + turn[:, rest + j : rest + j + 1] * rows[j : j + 1, :]
        here = slice(i * LANES, i * LANES + size)
        out[here, :LANES] = (packed[here, :] + term[:, :LANES]) * scale[:, :LANES]
        out[here, LANES:] = (turn[:, :rest] + term[:, LANES:]) * scale[:, LANES:]


def groups_of(axes, first):
    sizes = {axis: lax.axis_size(axis) for axis in ALL}
    places = np.arange(np.prod(list(sizes.values()))).reshape(*sizes.values())
    for axis, start in zip(axes, first, strict=True):
        places = np.roll(places, -start, ALL.index(axis))
    others = [i for i, axis in enumerate(ALL) if axis not in axes]
    places = places.transpose(*others, *(ALL.index(axis) for axis in axes))
    return places.reshape(-1, int(np.prod([sizes[axis] for axis in axes]))).tolist()


def exchanged(tiles, groups):
    pieces = tiles.reshape(len(groups[0]), -1)
    got = lax.all_to_all(
        pieces, ALL, split_axis=0, concat_axis=0, tiled=True, axis_index_groups=groups
    )
    return got.reshape(tiles.shape)


def step(snapshots, final_snapshot, pod_modes, right_vectors, inverse_sing, eigen_vectors):
    blocks = lax.axis_size("tm")
    rows, rank = snapshots.shape[0], right_vectors.shape[1]
    half = rows // (2 * blocks)
    place = lax.axis_index(("core", "tm")).astype(jnp.int32)[None]
    sing = inverse_sing[None, :]

    def sent(value, distance):
        return lax.ppermute(
            value,
            ("core", "tm"),
            [
                (core * blocks + i, core * blocks + (i + distance * (1 - 2 * core)) % blocks)
                for core in range(lax.axis_size("core"))
                for i in range(blocks)
            ],
        )

    near, far = lax.axis_size(NEAR), lax.axis_size(FAR)
    near_groups, far_groups = groups_of(NEAR, NEAR_FIRST), groups_of(FAR, FAR_FIRST)
    lines = rank + 2 * (rank - LANES + BLOCKS)
    size = lines // near
    packed, *snaps_in, final_in, vectors_in = call(
        term_kernel,
        (
            f32(lines, LANES),
            *[f32(2 * half, snapshots.shape[1])] * (BLOCKS - 1),
            f32(1, rows),
            f32(rank, snapshots.shape[1]),
        ),
        place,
        snapshots,
        final_snapshot[None, :],
        pod_modes.T,
        right_vectors.T,
        smem=1,
        hbm=(1, 2, 3, 4),
        scratch=(
            pltpu.VMEM((2 * half, snapshots.shape[1]), jnp.float32),
            pltpu.VMEM((rank, rows), jnp.float32),
            pltpu.SemaphoreType.DMA((2 * BLOCKS + 2,)),
        ),
    )
    tiles = exchanged(packed, near_groups)

    share = f32(rank + EXTRA, 2 * half)

    def share_for(distance):
        kernel = functools.partial(share_kernel, distance=distance)
        return call(kernel, share, place, snaps_in[distance - 1], final_in, vectors_in, smem=1)

    two_right, left, one_right = share_for(2), share_for(3), share_for(1)
    from_left = sent(two_right, 1)

    copied = functools.partial(sum_and_copy_kernel, size=size)
    tiles = call(functools.partial(copied, copies=far), f32(far * size, LANES), tiles)
    tiles = exchanged(tiles, far_groups)
    from_left = sent(call(add_kernel, share, one_right, from_left), 1)
    from_right = sent(left, -1)

    tiles = call(functools.partial(copied, copies=near), f32(near * size, LANES), tiles)
    tiles = exchanged(tiles, near_groups)
    own = call(
        own_share_kernel,
        share,
        place,
        snapshots,
        final_snapshot[None, :],
        right_vectors.T,
        smem=1,
        hbm=(1, 2, 3),
        scratch=(
            pltpu.VMEM((2 * half, snapshots.shape[1]), jnp.float32),
            pltpu.VMEM((1, 2 * half), jnp.float32),
            pltpu.VMEM((rank, snapshots.shape[1]), jnp.float32),
            pltpu.SemaphoreType.DMA((3,)),
        ),
    )
    dmd_modes, last_rows = call(
        dmd_kernel,
        (f32(rank, 2 * half), f32(BLOCKS, rank)),
        own,
        from_right,
        from_left,
        sing,
        eigen_vectors,
    )
    reduced_operator = call(operator_kernel, f32(rank, rank), tiles, last_rows, sing)
    return reduced_operator, dmd_modes.T


def solution(mesh):
    finer = Mesh(mesh.devices.reshape(4, 2, 4, 2, 2, mesh.shape["tm"]), (*SPACE, "tm"))
    return jax.shard_map(
        step,
        mesh=finer,
        in_specs=(P(SPACE, "tm"), P(SPACE), P(SPACE, None), P("tm", None), P(), P()),
        out_specs=(P(), P((*SPACE, "tm"), None)),
        check_vma=False,
    )
```

```python
import functools

import jax
import jax.numpy as jnp
import numpy as np
from jax import lax
from jax.experimental import pallas as pl
from jax.experimental.pallas import tpu as pltpu
from jax.sharding import Mesh
from jax.sharding import PartitionSpec as P

SPACE = ("y_far", "y_near", "z_far", "z_near", "core")
ALL = (*SPACE, "tm")
NEAR = ("y_near", "z_near", "core", "tm")
FAR = ("y_far", "z_far")
NEAR_FIRST = (0, 1, 1, 2)
FAR_FIRST = (3, 3)
LANES = 128
BLOCKS = 4
EXTRA = 2 * BLOCKS
VMEM_GRANT = 16 << 20


def f32(*shape):
    return jax.ShapeDtypeStruct(shape, jnp.float32)


def call(kernel, out, *args, smem=0, hbm=(), hbm_out=(), scratch=()):
    whole = pl.BlockSpec(memory_space=pltpu.VMEM)
    scalar = pl.BlockSpec(memory_space=pltpu.SMEM)
    outs = out if isinstance(out, tuple) else (out,)
    specs = [scalar] * smem + [whole] * (len(args) - smem)
    args = list(args)
    for i in hbm:
        specs[i] = pl.BlockSpec(memory_space=pltpu.HBM)
        args[i] = pltpu.with_memory_space_constraint(args[i], pltpu.HBM)
    result = pl.pallas_call(
        kernel,
        out_shape=outs,
        in_specs=specs,
        scratch_shapes=scratch,
        out_specs=[
            pl.BlockSpec(memory_space=pltpu.HBM) if i in hbm_out else whole for i in range(len(outs))
        ],
        compiler_params=pltpu.CompilerParams(vmem_limit_bytes=VMEM_GRANT),
    )(*args)
    return result if isinstance(out, tuple) else result[0]


def split(x):
    high = x.astype(jnp.bfloat16)
    return high, (x - high.astype(jnp.float32)).astype(jnp.bfloat16)


def three_pass(a, b, contract=(1, 1)):
    dims = (((contract[0],), (contract[1],)), ((), ()))
    dot = functools.partial(
        lax.dot_general, dimension_numbers=dims, preferred_element_type=jnp.float32
    )
    (a_high, a_low), (b_high, b_low) = a, b
    return dot(a_high, b_high) + (dot(a_high, b_low) + dot(a_low, b_high))


def block_and_step(place):
    return lax.rem(place, BLOCKS), 1 + (BLOCKS - 2) * lax.div(place, BLOCKS)


def shifted(vectors):
    lane = lax.broadcasted_iota(jnp.int32, vectors.shape, 1)
    return jnp.where(lane == 0, 0.0, pltpu.roll(vectors, 1, 1))


def turned(row):
    row = jnp.pad(row, ((0, 0), (0, 2 * LANES - row.shape[1])))
    halves = [
        jnp.broadcast_to(row[:, i * LANES : (i + 1) * LANES], (LANES, LANES)).T[:, :1]
        for i in range(2)
    ]
    return jnp.concatenate(halves, axis=0)


def term_kernel(
    place, snaps, final, modes, vectors, packed, first_in, second_in, third_in, final_in, vectors_in, own_in, modes_in, sems
):
    rank, _ = vectors.shape
    points = own_in.shape[0]
    block, step = block_and_step(place[0])
    held = (own_in, first_in, second_in, third_in)
    spans = [
        pl.ds(pl.multiple_of(lax.rem(block + i * step, BLOCKS) * points, points), points)
        for i in range(BLOCKS)
    ]
    got_modes = [
        pltpu.make_async_copy(modes.at[:, here], modes_in.at[:, pl.ds(i * points, points)], sems.at[i])
        for i, here in enumerate(spans)
    ]
    got_snaps = [
        pltpu.make_async_copy(snaps.at[here, :], held[i], sems.at[BLOCKS + i])
        for i, here in enumerate(spans)
    ]
    got_final = pltpu.make_async_copy(final, final_in, sems.at[2 * BLOCKS])
    got_vectors = pltpu.make_async_copy(vectors, vectors_in, sems.at[2 * BLOCKS + 1])
    got_vectors.start()
    got_final.start()
    for i in range(BLOCKS):
        got_modes[i].start()
        got_snaps[i].start()

    total = of_final = None
    got_vectors.wait()
    right = split(shifted(vectors_in[...]))
    got_final.wait()
    for i, here in enumerate(spans):
        got_modes[i].wait()
        got_snaps[i].wait()
        left, last = modes_in[:, i * points : (i + 1) * points], final_in[:, here]
        product = three_pass(split(left), split(held[i][...]), (1, 0))
        total = product if total is None else total + product
        for j in range(0, points, LANES):
            column = left[:, j : j + LANES] * last[:, j : j + LANES]
            of_final = column if of_final is None else of_final + column
    whole = three_pass(split(total), right)
    of_final = jnp.sum(of_final, axis=1, keepdims=True)
    first = jnp.where(block == 0, of_final, total[:, :1])
    packed[:rank, :] = whole[:, :LANES]
    rest = rank - LANES
    tail = jnp.pad(whole[:, LANES:], ((0, 0), (0, LANES - rest)))
    lane = lax.broadcasted_iota(jnp.int32, tail.shape, 1)
    tail = jnp.where(lane == rest + block, first, tail)
    tail = jnp.pad(tail, ((0, 2 * LANES - rank), (0, 0)))
    used = rest + BLOCKS
    for i in range(2):
        turn = tail[i * LANES : (i + 1) * LANES].T
        packed[rank + i * used : rank + (i + 1) * used, :] = turn[:used]


def shares_of(me, snaps, final, vectors):
    rank, snapshots = vectors.shape
    points = snaps.shape[0]
    row = lax.broadcasted_iota(jnp.int32, (EXTRA, snapshots), 0)
    column = lax.broadcasted_iota(jnp.int32, (EXTRA, snapshots), 1)
    unit = jnp.where((row == me) & (column == 0), 1.0, 0.0)
    left = split(jnp.concatenate([shifted(vectors), unit], axis=0))
    tail = jnp.pad(vectors[:, snapshots - LANES :], ((0, 2 * LANES - rank), (0, 0)))
    last = [tail[:LANES].T[LANES - 1 :], tail[LANES:].T[LANES - 1 :]]
    last = jnp.concatenate(last * (points // (2 * LANES)), axis=1)
    block = three_pass(left, split(snaps))
    slot = lax.broadcasted_iota(jnp.int32, (EXTRA, points), 0)
    extra = jnp.where((slot == me) & (me == 0), final, block[rank:])
    extra = jnp.where(slot == BLOCKS + lax.rem(me + 1, BLOCKS), last, extra)
    return block[:rank], extra


def share_kernel(place, snaps, final, vectors, out, *, distance):
    rank, points = vectors.shape[0], out.shape[1]
    block, step = block_and_step(place[0])
    owner = lax.rem(block + distance * step, BLOCKS)
    here = pl.ds(pl.multiple_of(owner * points, points), points)
    out[:rank, :], out[rank:, :] = shares_of(block, snaps[...], final[:, here], vectors[...])


def add_kernel(own, arrived, out):
    out[...] = own[...] + arrived[...]


def sum_and_copy_kernel(tiles, out, *, size, copies):
    total = tiles[:size, :]
    for i in range(1, tiles.shape[0] // size):
        total = total + tiles[i * size : (i + 1) * size, :]
    for i in range(copies):
        out[i * size : (i + 1) * size, :] = total


def own_share_kernel(place, snaps, final, vectors, out, snaps_in, final_in, vectors_in, sems):
    rank, points = vectors.shape[0], out.shape[1]
    block, _ = block_and_step(place[0])
    here = pl.ds(pl.multiple_of(block * points, points), points)
    copies = (
        pltpu.make_async_copy(vectors, vectors_in, sems.at[0]),
        pltpu.make_async_copy(snaps.at[here, :], snaps_in, sems.at[1]),
        pltpu.make_async_copy(final.at[:, here], final_in, sems.at[2]),
    )
    for copy in copies:
        copy.start()
    for copy in copies:
        copy.wait()
    out[:rank, :], out[rank:, :] = shares_of(block, snaps_in[...], final_in[...], vectors_in[...])


def dmd_kernel(own, from_right, from_left, sing, eigen, out, rows, done, sems):
    rank = out.shape[0]
    scale = turned(sing[...])[:rank]
    total = own[...] + from_right[...] + from_left[...]
    first = total[rank : rank + BLOCKS]
    last = total[rank + BLOCKS :, :rank]
    rows[...] = last
    summed = total[:rank] + three_pass(split(last), split(first), (0, 0))
    right = split(eigen[...])
    half = done.shape[1] // 2
    copies = []
    for i in range(2):
        there = pl.ds(i * half, half)
        done[:, there] = three_pass(right, split(summed[:, i * half : (i + 1) * half] * scale), (0, 0))
        copies.append(pltpu.make_async_copy(done.at[:, there], out.at[:, there], sems.at[i]))
        copies[i].start()
    for copy in copies:
        copy.wait()


def operator_kernel(packed, rows, sing, out):
    rank = out.shape[0]
    rest = rank - LANES
    used = rest + BLOCKS
    scale = sing[...]
    for i, size in ((0, LANES), (1, rest)):
        tail = packed[rank + i * used : rank + (i + 1) * used, :]
        turn = jnp.pad(tail, ((0, LANES - used), (0, 0))).T[:size]
        term = turn[:, rest : rest + 1] * rows[:1, :]
        for j in range(1, BLOCKS):
            term = term + turn[:, rest + j : rest + j + 1] * rows[j : j + 1, :]
        here = slice(i * LANES, i * LANES + size)
        out[here, :LANES] = (packed[here, :] + term[:, :LANES]) * scale[:, :LANES]
        out[here, LANES:] = (turn[:, :rest] + term[:, LANES:]) * scale[:, LANES:]


def groups_of(axes, first):
    sizes = {axis: lax.axis_size(axis) for axis in ALL}
    places = np.arange(np.prod(list(sizes.values()))).reshape(*sizes.values())
    for axis, start in zip(axes, first, strict=True):
        places = np.roll(places, -start, ALL.index(axis))
    others = [i for i, axis in enumerate(ALL) if axis not in axes]
    places = places.transpose(*others, *(ALL.index(axis) for axis in axes))
    return places.reshape(-1, int(np.prod([sizes[axis] for axis in axes]))).tolist()


def exchanged(tiles, groups):
    pieces = tiles.reshape(len(groups[0]), -1)
    got = lax.all_to_all(
        pieces, ALL, split_axis=0, concat_axis=0, tiled=True, axis_index_groups=groups
    )
    return got.reshape(tiles.shape)


def step(snapshots, final_snapshot, pod_modes, right_vectors, inverse_sing, eigen_vectors):
    blocks = lax.axis_size("tm")
    rows, rank = snapshots.shape[0], right_vectors.shape[1]
    half = rows // (2 * blocks)
    place = lax.axis_index(("core", "tm")).astype(jnp.int32)[None]
    sing = inverse_sing[None, :]

    def sent(value, distance):
        return lax.ppermute(
            value,
            ("core", "tm"),
            [
                (core * blocks + i, core * blocks + (i + distance * (1 - 2 * core)) % blocks)
                for core in range(lax.axis_size("core"))
                for i in range(blocks)
            ],
        )

    near, far = lax.axis_size(NEAR), lax.axis_size(FAR)
    near_groups, far_groups = groups_of(NEAR, NEAR_FIRST), groups_of(FAR, FAR_FIRST)
    lines = rank + 2 * (rank - LANES + BLOCKS)
    size = lines // near
    packed, *snaps_in, final_in, vectors_in = call(
        term_kernel,
        (
            f32(lines, LANES),
            *[f32(2 * half, snapshots.shape[1])] * (BLOCKS - 1),
            f32(1, rows),
            f32(rank, snapshots.shape[1]),
        ),
        place,
        snapshots,
        final_snapshot[None, :],
        pod_modes.T,
        right_vectors.T,
        smem=1,
        hbm=(1, 2, 3, 4),
        scratch=(
            pltpu.VMEM((2 * half, snapshots.shape[1]), jnp.float32),
            pltpu.VMEM((rank, rows), jnp.float32),
            pltpu.SemaphoreType.DMA((2 * BLOCKS + 2,)),
        ),
    )
    tiles = exchanged(packed, near_groups)

    share = f32(rank + EXTRA, 2 * half)

    def share_for(distance):
        kernel = functools.partial(share_kernel, distance=distance)
        return call(kernel, share, place, snaps_in[distance - 1], final_in, vectors_in, smem=1)

    two_right, left, one_right = share_for(2), share_for(3), share_for(1)
    from_left = sent(two_right, 1)

    copied = functools.partial(sum_and_copy_kernel, size=size)
    tiles = call(functools.partial(copied, copies=far), f32(far * size, LANES), tiles)
    tiles = exchanged(tiles, far_groups)
    from_left = sent(call(add_kernel, share, one_right, from_left), 1)
    from_right = sent(left, -1)

    tiles = call(functools.partial(copied, copies=near), f32(near * size, LANES), tiles)
    tiles = exchanged(tiles, near_groups)
    own = call(
        own_share_kernel,
        share,
        place,
        snapshots,
        final_snapshot[None, :],
        right_vectors.T,
        smem=1,
        hbm=(1, 2, 3),
        scratch=(
            pltpu.VMEM((2 * half, snapshots.shape[1]), jnp.float32),
            pltpu.VMEM((1, 2 * half), jnp.float32),
            pltpu.VMEM((rank, snapshots.shape[1]), jnp.float32),
            pltpu.SemaphoreType.DMA((3,)),
        ),
    )
    dmd_modes, last_rows = call(
        dmd_kernel,
        (f32(rank, 2 * half), f32(BLOCKS, rank)),
        own,
        from_right,
        from_left,
        sing,
        eigen_vectors,
        hbm_out=(0,),
        scratch=(
            pltpu.VMEM((rank, 2 * half), jnp.float32),
            pltpu.SemaphoreType.DMA((2,)),
        ),
    )
    reduced_operator = call(operator_kernel, f32(rank, rank), tiles, last_rows, sing)
    return reduced_operator, dmd_modes.T


def solution(mesh):
    finer = Mesh(mesh.devices.reshape(4, 2, 4, 2, 2, mesh.shape["tm"]), (*SPACE, "tm"))
    return jax.shard_map(
        step,
        mesh=finer,
        in_specs=(P(SPACE, "tm"), P(SPACE), P(SPACE, None), P("tm", None), P(), P()),
        out_specs=(P(), P((*SPACE, "tm"), None)),
        check_vma=False,
    )
```
